64 devices in a mesh: rep: 4 (over x, y), dp: 16 (over z, core).
Axes of the slice: x: 2, y: 2, z: 8, core: 2. Of those that a mesh axis runs over, the one named last changes fastest.
The devices are a block of a 4x4x8 slice.
Arguments:
- x: bfloat16 [64, 2048, 512], P(('rep', 'dp')), parts along dimension 0
- dy: bfloat16 [64, 2048, 512], P(('rep', 'dp')), parts along dimension 0
- wq: bfloat16 [2, 512, 512], P(None, 'dp')
- wk: bfloat16 [2, 512, 512], P(None, 'dp')
- wv: bfloat16 [2, 512, 512], P(None, 'dp')
- wo: bfloat16 [2, 512, 512], P(None, 'dp')
- w_gate: bfloat16 [2, 512, 2048], P(None, 'dp')
- w_up: bfloat16 [2, 512, 2048], P(None, 'dp')
- w_down: bfloat16 [2, 2048, 512], P(None, 'dp')
- m_wq: float32 [2, 512, 512], P(None, 'dp')
- m_wk: float32 [2, 512, 512], P(None, 'dp')
- m_wv: float32 [2, 512, 512], P(None, 'dp')
- m_wo: float32 [2, 512, 512], P(None, 'dp')
- m_w_gate: float32 [2, 512, 2048], P(None, 'dp')
- m_w_up: float32 [2, 512, 2048], P(None, 'dp')
- m_w_down: float32 [2, 2048, 512], P(None, 'dp')
- v_wq: float32 [2, 512, 512], P(None, 'dp')
- v_wk: float32 [2, 512, 512], P(None, 'dp')
- v_wv: float32 [2, 512, 512], P(None, 'dp')
- v_wo: float32 [2, 512, 512], P(None, 'dp')
- v_w_gate: float32 [2, 512, 2048], P(None, 'dp')
- v_w_up: float32 [2, 512, 2048], P(None, 'dp')
- v_w_down: float32 [2, 2048, 512], P(None, 'dp')
Outputs:
- output 1: bfloat16 [8, 512, 512], P('rep', 'dp'), parts along dimension 0
- output 2: bfloat16 [8, 512, 512], P('rep', 'dp'), parts along dimension 0
- output 3: bfloat16 [8, 512, 512], P('rep', 'dp'), parts along dimension 0
- output 4: bfloat16 [8, 512, 512], P('rep', 'dp'), parts along dimension 0
- output 5: bfloat16 [8, 512, 2048], P('rep', 'dp'), parts along dimension 0
- output 6: bfloat16 [8, 512, 2048], P('rep', 'dp'), parts along dimension 0
- output 7: bfloat16 [8, 2048, 512], P('rep', 'dp'), parts along dimension 0
- output 8: float32 [8, 512, 512], P('rep', 'dp'), parts along dimension 0
- output 9: float32 [8, 512, 512], P('rep', 'dp'), parts along dimension 0
- output 10: float32 [8, 512, 512], P('rep', 'dp'), parts along dimension 0
- output 11: float32 [8, 512, 512], P('rep', 'dp'), parts along dimension 0
- output 12: float32 [8, 512, 2048], P('rep', 'dp'), parts along dimension 0
- output 13: float32 [8, 512, 2048], P('rep', 'dp'), parts along dimension 0
- output 14: float32 [8, 2048, 512], P('rep', 'dp'), parts along dimension 0
- output 15: float32 [8, 512, 512], P('rep', 'dp'), parts along dimension 0
- output 16: float32 [8, 512, 512], P('rep', 'dp'), parts along dimension 0
- output 17: float32 [8, 512, 512], P('rep', 'dp'), parts along dimension 0
- output 18: float32 [8, 512, 512], P('rep', 'dp'), parts along dimension 0
- output 19: float32 [8, 512, 2048], P('rep', 'dp'), parts along dimension 0
- output 20: float32 [8, 512, 2048], P('rep', 'dp'), parts along dimension 0
- output 21: float32 [8, 2048, 512], P('rep', 'dp'), parts along dimension 0
There are 4 independent parts. The reference program is written for one: setup_inputs(seed, part) draws one part's arguments, and reference() takes and returns one part's arrays. A program takes and returns all parts, laid end to end along the dimension named above; an argument that names none is the same for every part.
All inputs are finite; a program needn't handle non-finite values.
Results may differ from the reference program's by a relative error of at most 0.024.
Values are sent between devices in bfloat16 or wider.
A program may use at most 768 MiB of HBM per device.

```python
import jax
import jax.numpy as jnp
from jax import lax

SEQUENCES = 16
TOKENS = 2048
D = 512
HEADS = 2
KV_HEADS = 2
HEAD = 256
FF = 2048
LAYERS = 2
THETA = 10000
NAMES = ("wq", "wk", "wv", "wo", "w_gate", "w_up", "w_down")
SHAPES = {
    "wq": (LAYERS, D, HEADS * HEAD),
    "wk": (LAYERS, D, KV_HEADS * HEAD),
    "wv": (LAYERS, D, KV_HEADS * HEAD),
    "wo": (LAYERS, HEADS * HEAD, D),
    "w_gate": (LAYERS, D, FF),
    "w_up": (LAYERS, D, FF),
    "w_down": (LAYERS, FF, D),
}


def bump(key, n, height):
    away = (jnp.arange(n, dtype=jnp.int32) - jax.random.randint(key, (), 0, n, jnp.int32)) % n
    return jnp.where(away < n // 8, height, 1.0)


def together(key, own, strength):
    shared = jax.random.normal(key, own.shape[1:], jnp.float32)
    return (own + strength * shared) * lax.rsqrt(1 + strength * strength)


def setup_inputs(seed: int = 0, part: int = 0) -> dict:
    kx, kdy, ka, kb, kz, kf, kh, kl, *keys = jax.random.split(jax.random.key(seed), 8 + 3 * len(NAMES))
    kx, kdy, ka, kb = (jax.random.fold_in(k, part) for k in (kx, kdy, ka, kb))
    kw, km, kv = (keys[i::3] for i in range(3))
    shape = (SEQUENCES, TOKENS, D)
    much_x, much_dy = jax.random.uniform(kz, (2,), jnp.float32, 0.0, 1.0)
    loud = 2.0 ** jax.random.uniform(jax.random.fold_in(kz, 1), (), jnp.float32, -1.0, 2.0)
    layers = 2.0 ** jax.random.uniform(kl, (LAYERS, 1, 1), jnp.float32, -1.0, 1.0)
    times = {"wq": 1.0, "wk": 1.0, "wv": 2.0, "wo": layers, "w_gate": 1.0, "w_up": bump(kh, FF, 4.0), "w_down": layers}
    x = together(ka, jax.random.normal(kx, shape, jnp.float32), much_x) * bump(kf, D, 4.0)
    dy = together(kb, jax.random.normal(kdy, shape, jnp.float32), much_dy)
    drawn = {"x": x.astype(jnp.bfloat16), "dy": (loud * dy * (SEQUENCES * TOKENS) ** -0.5).astype(jnp.bfloat16)}
    for key, name in zip(kw, NAMES, strict=True):
        drawn[name] = (jax.random.normal(key, SHAPES[name], jnp.float32) * SHAPES[name][1] ** -0.5 * times[name]).astype(jnp.bfloat16)
    for key, name in zip(km, NAMES, strict=True):
        drawn[f"m_{name}"] = 0.1 * jax.random.normal(key, SHAPES[name], jnp.float32)
    for key, name in zip(kv, NAMES, strict=True):
        drawn[f"v_{name}"] = loud * loud * jax.random.uniform(key, SHAPES[name], jnp.float32, 0.2, 0.6)
    return drawn


def matmul(a, w):
    return jnp.dot(a, w, preferred_element_type=jnp.float32).astype(jnp.bfloat16)


def normed(h):
    wide = h.astype(jnp.float32)
    scale = lax.rsqrt(jnp.mean(wide**2, -1, keepdims=True) + 1e-6)
    return (wide * scale).astype(jnp.bfloat16)


def turned(t, theta):
    half = t.shape[-1] // 2
    angle = jnp.arange(t.shape[0], dtype=jnp.float32)[:, None] * theta ** (-jnp.arange(half, dtype=jnp.float32) / half)
    cos, sin = jnp.cos(angle)[:, None], jnp.sin(angle)[:, None]
    a, b = t[..., :half].astype(jnp.float32), t[..., half:].astype(jnp.float32)
    return jnp.concatenate([a * cos - b * sin, b * cos + a * sin], -1).astype(jnp.bfloat16)


def seen_by(q, k, v):
    tokens, kv = q.shape[0], k.shape[1]
    q = q.reshape(tokens, kv, -1, q.shape[-1])
    scores = jnp.einsum("tgsd,ugd->gstu", q.astype(jnp.float32), k.astype(jnp.float32)) * q.shape[-1] ** -0.5
    place = jnp.arange(tokens)
    weights = jax.nn.softmax(jnp.where(place[:, None] >= place, scores, -jnp.inf), -1).astype(jnp.bfloat16)
    return jnp.einsum("gstu,ugd->tgsd", weights.astype(jnp.float32), v.astype(jnp.float32)).astype(jnp.bfloat16).reshape(tokens, -1)


def layer(h, w):
    a = normed(h)
    q, k = (turned(matmul(a, w[name]).reshape(h.shape[0], -1, HEAD), THETA) for name in ("wq", "wk"))
    h = h + matmul(seen_by(q, k, matmul(a, w["wv"]).reshape(h.shape[0], -1, HEAD)), w["wo"])
    b = normed(h)
    gate = jnp.dot(b, w["w_gate"], preferred_element_type=jnp.float32)
    up = jnp.dot(b, w["w_up"], preferred_element_type=jnp.float32)
    return h + matmul((jax.nn.silu(gate) * up).astype(jnp.bfloat16), w["w_down"])


def adamw(w, m, v, g):
    m = 0.9 * m + 0.1 * g
    v = 0.95 * v + 0.05 * g * g
    step = m * lax.rsqrt(v + 1e-8) + 0.1 * w
    return (w - 0.02 * step).astype(jnp.bfloat16), m, v


def stack(weights, h):
    return lax.scan(lambda h, w: (layer(h, w), None), h, weights)[0]


def reference(x, dy, wq, wk, wv, wo, w_gate, w_up, w_down, m_wq, m_wk, m_wv, m_wo, m_w_gate, m_w_up, m_w_down, v_wq, v_wk, v_wv, v_wo, v_w_gate, v_w_up, v_w_down):
    weights = dict(zip(NAMES, (wq, wk, wv, wo, w_gate, w_up, w_down), strict=True))

    def take(so_far, sequence):
        h, by_y = sequence
        _, back = jax.vjp(stack, weights, h)
        by_weights, by_h = back(by_y)
        return jax.tree.map(lambda total, term: total + term.astype(jnp.float32), so_far, by_weights), by_h

    none_yet = {name: jnp.zeros(w.shape, jnp.float32) for name, w in weights.items()}
    by_weights, by_x = lax.scan(take, none_yet, (x, dy))
    gradients = [by_weights[name].astype(jnp.bfloat16).astype(jnp.float32) for name in NAMES]
    first = (m_wq, m_wk, m_wv, m_wo, m_w_gate, m_w_up, m_w_down)
    second = (v_wq, v_wk, v_wv, v_wo, v_w_gate, v_w_up, v_w_down)
    new = [adamw(weights[name].astype(jnp.float32), m, v, g) for name, m, v, g in zip(NAMES, first, second, gradients, strict=True)]
    return tuple(one[which] for which in range(3) for one in new)
```

```python
import functools

import jax
import jax.numpy as jnp
import numpy as np
from jax import lax
from jax.experimental import pallas as pl
from jax.experimental.pallas import tpu as pltpu
from jax.sharding import PartitionSpec as P

HEAD = 256
THETA = 10000
NAMES = ("wq", "wk", "wv", "wo", "w_gate", "w_up", "w_down")
LOG2E = 1.4426950408889634
NEG = -1e30
MIB = 2**20
MESH = pl.DeviceIdType.MESH
bf16, f32 = jnp.bfloat16, jnp.float32
ANY = pl.BlockSpec(memory_space=pl.ANY)
VMEM = pl.BlockSpec(memory_space=pltpu.VMEM)


def dot(a, b, ca=1, cb=0):
    return lax.dot_general(a, b, (((ca,), (cb,)), ((), ())), preferred_element_type=f32)


def sds(shape, dtype):
    return jax.ShapeDtypeStruct(shape, dtype)


class Place:
    def __init__(self, devices):
        me = lax.axis_index("dp")
        self.me, self.chips = me, devices // 2
        self.z, self.c = me // 2, lax.rem(me, 2)
        self.right = lax.rem(me + 2, devices)
        self.left = lax.rem(me + devices - 2, devices)
        self.partner = me + 1 - 2 * self.c

    def chip(self, away):
        return lax.rem(self.z + (away + self.chips), self.chips)


def hops(devices, flip):
    chips = devices // 2
    far, near = chips // 2, chips - 1 - chips // 2
    return (near, far) if flip else (far, near)


def meet(devices):
    p = Place(devices)
    barrier = pltpu.get_barrier_semaphore()
    for other in (p.left, p.right, p.partner):
        pl.semaphore_signal(barrier, inc=1, device_id={"dp": other}, device_id_type=MESH)
    pl.semaphore_wait(barrier, 3)


class Gather:
    def __init__(self, devices, shards, layer, outs, where):
        self.devices, self.layer, self.where = devices, layer, where
        self.ins = list(shards)
        self.in_specs = [
            pl.BlockSpec((1,) + s.shape[1:], lambda *_: (layer, 0, 0)) for s in shards
        ]
        self.outs = outs
        self.out_specs = [ANY] * len(outs)
        self.units = len(shards)
        slots = 2 * (devices // 2) + 1
        self.scratch = [
            pltpu.SemaphoreType.DMA((self.units, slots)),
            pltpu.SemaphoreType.DMA((self.units, slots)),
            pltpu.SemaphoreType.DMA((self.units,)),
        ]

    def bind(self, ins, outs, scratch):
        self.rows, self.full = ins, outs
        self.send, self.recv, self.local = scratch

    def view(self, u, device):
        out, index = self.where[u]
        r = self.ins[u].shape[1]
        rows = pl.ds(pl.multiple_of(device * r, r), r)
        return self.full[out].at[rows, :] if index is None else self.full[out].at[index, rows, :]

    def copy(self, u, slot, source, device, to):
        return pltpu.make_async_remote_copy(
            src_ref=source, dst_ref=self.view(u, device), send_sem=self.send.at[u, slot], recv_sem=self.recv.at[u, slot],
            device_id={"dp": to}, device_id_type=MESH)

    def flows(self, u):
        right, left = hops(self.devices, u % 2)
        half = self.devices // 4
        return (right, 0, 2 * half, 1), (left, half, 3 * half, -1)

    def first(self, u):
        p = Place(self.devices)
        own = self.rows[u].at[0]
        pltpu.make_async_copy(own, self.view(u, p.me), self.local.at[u]).start()
        (_, a, _, _), (_, b, _, _) = self.flows(u)
        self.copy(u, a, own, p.me, p.right).start()
        self.copy(u, b, own, p.me, p.left).start()
        self.copy(u, self.devices, own, p.me, p.partner).start()

    def hop(self, u, s):
        p = Place(self.devices)
        for count, ring, across, way in self.flows(u):
            if s > count:
                continue
            device = 2 * p.chip(-way * s) + p.c
            here = self.view(u, device)
            to = p.right if way == 1 else p.left
            self.copy(u, ring + s - 1, here, device, to).wait_recv()
            if s < count:
                self.copy(u, ring + s, here, device, to).start()
            self.copy(u, across + s - 1, here, device, p.partner).start()

    def last(self, u):
        p = Place(self.devices)
        own = self.rows[u].at[0]
        pltpu.make_async_copy(own, self.view(u, p.me), self.local.at[u]).wait()
        self.copy(u, self.devices, own, p.partner, p.partner).wait_recv()
        self.copy(u, self.devices, own, p.me, p.partner).wait_send()
        for count, ring, across, way in self.flows(u):
            to = p.right if way == 1 else p.left
            for s in range(1, count + 1):
                device = 2 * p.chip(-way * s) + p.c
                theirs = 2 * p.chip(-way * s) + 1 - p.c
                self.copy(u, across + s - 1, self.view(u, theirs), theirs, p.partner).wait_recv()
                self.copy(u, across + s - 1, self.view(u, device), device, p.partner).wait_send()
                self.copy(u, ring + s - 1, self.view(u, device), device, to).wait_send()

    def steps(self):
        most = max(hops(self.devices, 0))
        units = range(self.units)
        out = [functools.partial(self.first, u) for u in units]
        for s in range(1, most + 1):
            out += [functools.partial(self.hop, u, s) for u in units]
        return out, [functools.partial(self.last, u) for u in units]


class Scatter:
    def __init__(self, devices, terms):
        self.devices = devices
        self.ins = list(terms)
        self.in_specs = [ANY] * len(terms)
        self.units = len(terms)
        self.outs, self.out_specs, self.scratch = [], [], []
        chips = devices // 2
        for t in terms:
            m, _, _, r, n = t.shape
            self.outs.append(sds((m, r, n), bf16))
            self.out_specs.append(pl.BlockSpec((m, r, n), lambda *_: (0, 0, 0)))
            self.scratch += [
                pltpu.VMEM((m, chips, r, n), bf16),
                pltpu.VMEM((m, chips, r, n), bf16),
                pltpu.VMEM((chips, m, r, n), bf16),
                pltpu.VMEM((chips, m, r, n), bf16),
            ]
        self.scratch += [
            pltpu.SemaphoreType.DMA((self.units, chips + 1)),
            pltpu.SemaphoreType.DMA((self.units, chips + 1)),
            pltpu.SemaphoreType.DMA((self.units,)),
        ]

    def bind(self, ins, outs, scratch):
        self.terms, self.result = ins, outs
        self.own = scratch[0 : 4 * self.units : 4]
        self.pair = scratch[1 : 4 * self.units : 4]
        self.come = scratch[2 : 4 * self.units : 4]
        self.gone = scratch[3 : 4 * self.units : 4]
        self.send, self.recv, self.local = scratch[4 * self.units :]

    def flows(self, u):
        right, left = hops(self.devices, u % 2)
        return (right, 0, 1), (left, self.devices // 4, -1)

    def mine(self, u, p):
        return pltpu.make_async_copy(self.terms[u].at[:, :, p.c], self.own[u], self.local.at[u])

    def swap(self, u, p):
        slot = self.devices // 2
        return pltpu.make_async_remote_copy(
            src_ref=self.terms[u].at[:, :, 1 - p.c], dst_ref=self.pair[u], send_sem=self.send.at[u, slot], recv_sem=self.recv.at[u, slot],
            device_id={"dp": p.partner}, device_id_type=MESH)

    def copy(self, u, slot, to):
        return pltpu.make_async_remote_copy(
            src_ref=self.gone[u].at[slot], dst_ref=self.come[u].at[slot], send_sem=self.send.at[u, slot], recv_sem=self.recv.at[u, slot],
            device_id={"dp": to}, device_id_type=MESH)

    def first(self, u):
        p = Place(self.devices)
        self.mine(u, p).start()
        self.swap(u, p).start()

    def both(self, u, i, chip):
        return self.own[u][i, chip].astype(f32) + self.pair[u][i, chip].astype(f32)

    def hop(self, u, s):
        p = Place(self.devices)
        if s == 1:
            self.mine(u, p).wait()
            self.swap(u, p).wait_recv()
        for count, slot, way in self.flows(u):
            if s > count:
                continue
            to = p.right if way == 1 else p.left
            chip = p.chip(way * (count - s + 1))
            if s > 1:
                self.copy(u, slot + s - 2, to).wait_recv()
            for i in range(self.ins[u].shape[0]):
                total = self.both(u, i, chip)
                if s > 1:
                    total += self.come[u][slot + s - 2, i].astype(f32)
                self.gone[u][slot + s - 1, i] = total.astype(bf16)
            self.copy(u, slot + s - 1, to).start()

    def last(self, u):
        p = Place(self.devices)
        self.swap(u, p).wait_send()
        for count, slot, way in self.flows(u):
            to = p.right if way == 1 else p.left
            self.copy(u, slot + count - 1, to).wait_recv()
            for s in range(count):
                self.copy(u, slot + s, to).wait_send()
        for i in range(self.ins[u].shape[0]):
            total = self.both(u, i, p.z)
            for count, slot, _ in self.flows(u):
                total += self.come[u][slot + count - 1, i].astype(f32)
            self.result[u][i] = total.astype(bf16)

    def steps(self):
        most = max(hops(self.devices, 0))
        units = range(self.units)
        out = [functools.partial(self.first, u) for u in units]
        for s in range(1, most + 1):
            out += [functools.partial(self.hop, u, s) for u in units]
        return out, [functools.partial(self.last, u) for u in units]


def run(body, grid, ins, in_specs, outs, out_specs, scratch=(), side=None, ident=None, vmem=60, flops=0, name=None):
    counts = [len(ins), len(side.ins) if side else 0, len(outs), len(side.outs) if side else 0, len(scratch), len(side.scratch) if side else 0]
    total = int(np.prod(grid))

    def kernel(*refs):
        parts, at = [], 0
        for n in counts:
            parts.append(list(refs[at : at + n]))
            at += n
        step = pl.program_id(0)
        for axis in range(1, len(grid)):
            step = step * grid[axis] + pl.program_id(axis)
        end = []
        if side:
            side.bind(parts[1], parts[3], parts[5])
            todo, end = side.steps()
            due = {}
            for i, one in enumerate(todo):
                due.setdefault(i * total // len(todo), []).append(one)
            for at, some in sorted(due.items()):

                @pl.when(step == at)
                def _():
                    if at == 0:
                        meet(side.devices)
                    for one in some:
                        one()

        if body:
            body(*parts[0], *parts[2], *parts[4])
        if side:

            @pl.when(step == total - 1)
            def _():
                for one in end:
                    one()

    got = pl.pallas_call(
        kernel,
        grid=grid,
        in_specs=list(in_specs) + (side.in_specs if side else []),
        out_specs=list(out_specs) + (side.out_specs if side else []),
        out_shape=list(outs) + (side.outs if side else []),
        scratch_shapes=list(scratch) + (side.scratch if side else []),
        compiler_params=pltpu.CompilerParams(
            dimension_semantics=("arbitrary",) * len(grid), vmem_limit_bytes=vmem * MIB,
            **(dict(collective_id=ident, has_side_effects=True) if side else {})),
        cost_estimate=pl.CostEstimate(flops=flops, bytes_accessed=sum(a.size * a.dtype.itemsize for a in (*ins, *outs)), transcendentals=0),
        name=name,
    )(*ins, *(side.ins if side else []))
    return got[: len(outs)], got[len(outs) :]


def scale_of(wide):
    return lax.rsqrt(jnp.mean(wide * wide, -1, keepdims=True) + 1e-6)


def turn(t, cos, sin):
    half = t.shape[-1] // 2
    a, b = t[:, :half].astype(f32), t[:, half:].astype(f32)
    return jnp.concatenate([a * cos - b * sin, b * cos + a * sin], -1).astype(bf16)


def table(tokens):
    half = HEAD // 2
    angle = np.arange(tokens, dtype=np.float32)[:, None] * np.power(np.float32(THETA), -np.arange(half, dtype=np.float32) / np.float32(half))
    return jnp.asarray(np.cos(angle).astype(np.float32)), jnp.asarray(np.sin(angle).astype(np.float32))


def whole(shape):
    return pl.BlockSpec(shape, lambda *_: (0,) * len(shape))


def tiles(rows, columns):
    return pl.BlockSpec((rows, columns), lambda i, *_: (i, 0))


def project(h, qkvo, cos, sin, side=None, ident=None):
    tokens, d = h.shape
    heads = qkvo.shape[2] // HEAD
    tile = 512

    def body(h_ref, w_ref, cos_ref, sin_ref, *outs):
        wide = h_ref[...].astype(f32)
        a = (wide * scale_of(wide)).astype(bf16)
        for i, out in enumerate(outs):
            t = dot(a, w_ref[i]).astype(bf16)
            for n in range(heads):
                one = t[:, n * HEAD : (n + 1) * HEAD]
                out[n] = one if i == 2 else turn(one, cos_ref[...], sin_ref[...])

    out = pl.BlockSpec((heads, tile, HEAD), lambda i: (0, i, 0))
    return run(
        body, (tokens // tile,), [h, qkvo, cos, sin],
        [tiles(tile, d), whole(qkvo.shape), tiles(tile, HEAD // 2), tiles(tile, HEAD // 2)],
        [sds((heads, tokens, HEAD), bf16)] * 3, [out] * 3, side=side, ident=ident, flops=6 * tokens * d * heads * HEAD, name="project")


def attend(q, k, v, side=None, ident=None):
    heads, tokens, _ = q.shape
    b = 512
    e = HEAD**-0.5 * LOG2E

    def body(q_ref, k_ref, v_ref, o_ref, lse_ref, top_s, mix_s):
        iq = pl.program_id(0)
        top_s[...] = jnp.full(top_s.shape, NEG, f32)
        mix_s[...] = jnp.zeros(mix_s.shape, f32)
        ones = jnp.ones((8, b), bf16)

        def block(j, masked):
            here = pl.ds(pl.multiple_of(j * b, b), b)
            scores = [dot(k_ref[n, here, :], q_ref[n], 1, 1) for n in range(heads)]
            weights, keeps = [], []
            for n, s in enumerate(scores):
                if masked:
                    seen = lax.broadcasted_iota(jnp.int32, (b, b), 0) <= lax.broadcasted_iota(jnp.int32, (b, b), 1)
                    s = jnp.where(seen, s, 2 * NEG)
                old = top_s[n : n + 1, :]
                top = jnp.maximum(old, s.max(axis=0, keepdims=True))
                top_s[n : n + 1, :] = top
                weights.append(jnp.exp2((s - top) * e).astype(bf16))
                keeps.append(jnp.exp2((old - top) * e))
            for n in range(heads):
                values = jnp.concatenate([v_ref[n, here, :].T, ones], axis=0)
                mix_s[n] = mix_s[n] * keeps[n] + dot(values, weights[n])

        lax.fori_loop(0, iq, lambda j, _: block(j, False), None)
        block(iq, True)
        for n in range(heads):
            total = mix_s[n, HEAD : HEAD + 1, :]
            o_ref[:, n * HEAD : (n + 1) * HEAD] = (mix_s[n, :HEAD, :] * (1 / total)).T.astype(bf16)
            lse_ref[n : n + 1, :] = top_s[n : n + 1, :] * HEAD**-0.5 + jnp.log(total)

    keys = whole((heads, tokens, HEAD))
    return run(
        body, (tokens // b,), [q, k, v], [pl.BlockSpec((heads, b, HEAD), lambda i: (0, i, 0)), keys, keys],
        [sds((tokens, heads * HEAD), bf16), sds((heads, tokens), f32)],
        [tiles(b, heads * HEAD), pl.BlockSpec((heads, b), lambda i: (0, i))],
        [pltpu.VMEM((heads, b), f32), pltpu.VMEM((heads, HEAD + 8, b), f32)],
        side=side, ident=ident, flops=2 * heads * tokens * tokens * HEAD, name="attend")


def feed(h, o, qkvo, gate_w, up_w, down_w, last, side=None, ident=None):
    tokens, d = h.shape
    ff = gate_w.shape[1]
    tile, part = 512, 512

    def body(h_ref, o_ref, wo_ref, g_ref, u_ref, d_ref, h1_ref, gate_ref, up_ref, *rest):
        h1 = h_ref[...] + dot(o_ref[...], wo_ref[0]).astype(bf16)
        h1_ref[...] = h1
        wide = h1.astype(f32)
        b = (wide * scale_of(wide)).astype(bf16)
        total = None
        for at in range(0, ff, part):
            gate = dot(b, g_ref[:, at : at + part])
            up = dot(b, u_ref[:, at : at + part])
            gate_ref[:, at : at + part] = gate
            up_ref[:, at : at + part] = up
            if rest:
                p = (gate * jax.nn.sigmoid(gate) * up).astype(bf16)
                one = dot(p, d_ref[at : at + part, :])
                total = one if total is None else total + one
        if rest:
            rest[0][...] = h1 + total.astype(bf16)

    once = lambda shape: pl.BlockSpec(shape, lambda i: (0,) * len(shape), pipeline_mode=pl.Buffered(1))
    rows = tiles(tile, d)
    return run(
        body, (tokens // tile,), [h, o, qkvo, gate_w, up_w, down_w],
        [rows, tiles(tile, o.shape[1]), pl.BlockSpec((1,) + qkvo.shape[1:], lambda i: (3, 0, 0)), once(gate_w.shape), once(up_w.shape), once(down_w.shape)],
        [sds((tokens, d), bf16), sds((tokens, ff), f32), sds((tokens, ff), f32)] + ([] if last else [sds((tokens, d), bf16)]),
        [rows, tiles(tile, ff), tiles(tile, ff)] + ([] if last else [rows]),
        side=side, ident=ident, flops=2 * tokens * d * (d + 3 * ff), name="feed")


def feed_back(h1, gate, up, dh2, gate_w, up_w, down_w, side=None, ident=None):
    tokens, d = h1.shape
    ff = gate.shape[1]
    part, tile = 256, 512
    steps = ff // part

    def body(h1_ref, gate_ref, up_ref, dh2_ref, g_ref, u_ref, d_ref, dh1_ref, dg_ref, du_ref, dd_ref, b_s, p_s, dgate_s, dup_s, db_s):
        f = pl.program_id(0)

        @pl.when(f == 0)
        def _():
            for t in range(0, tokens, tile):
                wide = h1_ref[t : t + tile, :].astype(f32)
                b_s[t : t + tile, :] = (wide * scale_of(wide)).astype(bf16)
                db_s[t : t + tile, :] = jnp.zeros((tile, d), f32)

        for t in range(0, tokens, tile):
            here = slice(t, t + tile)
            dp = dot(dh2_ref[here, :], d_ref[...], 1, 1).astype(bf16).astype(f32)
            gate, up = gate_ref[here, :], up_ref[here, :]
            s = jax.nn.sigmoid(gate)
            soft = gate * s
            p_s[here, :] = (soft * up).astype(bf16)
            dup = (dp * soft).astype(bf16)
            dgate = (dp * up * (s + soft * (1 - s))).astype(bf16)
            dup_s[here, :] = dup
            dgate_s[here, :] = dgate
            db_s[here, :] += dot(dgate, g_ref[...], 1, 1) + dot(dup, u_ref[...], 1, 1)
        dd_ref[...] = dot(p_s[...], dh2_ref[...], 0, 0).astype(bf16)
        dg_ref[...] = dot(b_s[...], dgate_s[...], 0, 0).astype(bf16)
        du_ref[...] = dot(b_s[...], dup_s[...], 0, 0).astype(bf16)

        @pl.when(f == steps - 1)
        def _():
            for t in range(0, tokens, tile):
                here = slice(t, t + tile)
                wide = h1_ref[here, :].astype(f32)
                dn = db_s[here, :].astype(bf16).astype(f32)
                scale = scale_of(wide)
                back = scale * dn - wide * (scale * scale * scale * jnp.mean(dn * wide, -1, keepdims=True))
                dh1_ref[here, :] = dh2_ref[here, :] + back.astype(bf16)

    columns = lambda rows: pl.BlockSpec((rows, part), lambda f: (0, f))
    down = pl.BlockSpec((part, d), lambda f: (f, 0))
    return run(
        body, (steps,), [h1, gate, up, dh2, gate_w, up_w, down_w],
        [whole((tokens, d)), columns(tokens), columns(tokens), whole((tokens, d)), columns(d), columns(d), down],
        [sds((tokens, d), bf16), sds((d, ff), bf16), sds((d, ff), bf16), sds((ff, d), bf16)],
        [whole((tokens, d)), columns(d), columns(d), down],
        [pltpu.VMEM((tokens, d), bf16)] + [pltpu.VMEM((tokens, part), bf16)] * 3 + [pltpu.VMEM((tokens, d), f32)],
        side=side, ident=ident, flops=12 * tokens * d * ff, name="feed_back")


def out_back(dh1, o, qkvo, heads, side=None, ident=None):
    tokens, d = dh1.shape
    width = o.shape[1]
    tile = 512
    steps = tokens // tile

    def body(dh1_ref, o_ref, w_ref, do_ref, delta_ref, dw_ref, dw_s):
        i = pl.program_id(0)
        do = dot(dh1_ref[...], w_ref[0], 1, 1).astype(bf16)
        do_ref[...] = do
        for n in range(heads):
            cut = slice(n * HEAD, (n + 1) * HEAD)
            both = do[:, cut].astype(f32) * o_ref[:, cut].astype(f32)
            delta_ref[n : n + 1, :] = both.T.sum(axis=0, keepdims=True)
        one = dot(o_ref[...], dh1_ref[...], 0, 0)

        @pl.when(i == 0)
        def _():
            dw_s[...] = one

        @pl.when(i > 0)
        def _():
            dw_s[...] += one

        @pl.when(i == steps - 1)
        def _():
            dw_ref[...] = dw_s[...].astype(bf16)

    return run(
        body, (steps,), [dh1, o, qkvo],
        [tiles(tile, d), tiles(tile, width), pl.BlockSpec((1,) + qkvo.shape[1:], lambda i: (3, 0, 0))],
        [sds((tokens, width), bf16), sds((heads, tokens), f32), sds((width, d), bf16)],
        [tiles(tile, width), pl.BlockSpec((heads, tile), lambda i: (0, i)), whole((width, d))],
        [pltpu.VMEM((width, d), f32)], side=side, ident=ident, flops=4 * tokens * d * width, name="out_back")


def attend_back(q, k, v, do, lse, delta, side=None, ident=None):
    heads, tokens, _ = q.shape
    b = 512
    scale = HEAD**-0.5
    e = scale * LOG2E
    steps = tokens // b

    def body(q_ref, k_ref, v_ref, do_ref, lse_ref, delta_ref, dq_ref, dk_ref, dv_ref, dq_s, dk_s, dv_s):
        iq = pl.program_id(0)

        @pl.when(iq == 0)
        def _():
            dk_s[...] = jnp.zeros(dk_s.shape, f32)
            dv_s[...] = jnp.zeros(dv_s.shape, f32)

        dq_s[...] = jnp.zeros(dq_s.shape, f32)

        def block(j, masked):
            here = pl.ds(pl.multiple_of(j * b, b), b)
            dos = [do_ref[:, n * HEAD : (n + 1) * HEAD] for n in range(heads)]
            scores = [dot(k_ref[n, here, :], q_ref[n], 1, 1) for n in range(heads)]
            dps = [dot(v_ref[n, here, :], dos[n], 1, 1) for n in range(heads)]
            for n in range(heads):
                p = jnp.exp2(scores[n] * e - lse_ref[n : n + 1, :] * LOG2E)
                if masked:
                    seen = lax.broadcasted_iota(jnp.int32, (b, b), 0) <= lax.broadcasted_iota(jnp.int32, (b, b), 1)
                    p = jnp.where(seen, p, 0.0)
                ds = (p * (dps[n] - delta_ref[n : n + 1, :])).astype(bf16)
                dv_s[n, here, :] += dot(p.astype(bf16), dos[n])
                dk_s[n, here, :] += dot(ds, q_ref[n])
                dq_s[n] += dot(k_ref[n, here, :].T, ds)

        lax.fori_loop(0, iq, lambda j, _: block(j, False), None)
        block(iq, True)
        for n in range(heads):
            dq_ref[n] = (dq_s[n] * scale).T.astype(bf16)

        @pl.when(iq == steps - 1)
        def _():
            dk_ref[...] = (dk_s[...] * scale).astype(bf16)
            dv_ref[...] = dv_s[...].astype(bf16)

    keys = whole((heads, tokens, HEAD))
    queries = pl.BlockSpec((heads, b, HEAD), lambda i: (0, i, 0))
    stats = pl.BlockSpec((heads, b), lambda i: (0, i))
    return run(
        body, (steps,), [q, k, v, do, lse, delta], [queries, keys, keys, tiles(b, heads * HEAD), stats, stats],
        [sds((heads, tokens, HEAD), bf16)] * 3, [queries, keys, keys],
        [pltpu.VMEM((heads, HEAD, b), f32), pltpu.VMEM((heads, tokens, HEAD), f32), pltpu.VMEM((heads, tokens, HEAD), f32)],
        side=side, ident=ident, flops=5 * heads * tokens * tokens * HEAD, name="attend_back")


def project_back(h, dq, dk, dv, cos, sin, dh1, qkvo, first, side=None, ident=None):
    tokens, d = h.shape
    heads = dq.shape[0]
    width = heads * HEAD
    tile = 512
    steps = tokens // tile

    def body(h_ref, dq_ref, dk_ref, dv_ref, cos_ref, sin_ref, *rest):
        if first:
            dw_ref, dw_s = rest
        else:
            dh1_ref, w_ref, dw_ref, dh_ref, dw_s = rest
        i = pl.program_id(0)
        wide = h_ref[...].astype(f32)
        scale = scale_of(wide)
        a = (wide * scale).astype(bf16)
        back = None
        for n, ref in enumerate((dq_ref, dk_ref, dv_ref)):
            if n < 2:
                t = jnp.concatenate([turn(ref[m], cos_ref[...], -sin_ref[...]) for m in range(heads)], axis=1)
            else:
                t = jnp.concatenate([ref[m] for m in range(heads)], axis=1)
            one = dot(a, t, 0, 0)

            @pl.when(i == 0)
            def _():
                dw_s[n] = one

            @pl.when(i > 0)
            def _():
                dw_s[n] += one

            if not first:
                part = dot(t, w_ref[n], 1, 1)
                back = part if back is None else back + part
        if not first:
            dn = back.astype(bf16).astype(f32)
            back = scale * dn - wide * (scale * scale * scale * jnp.mean(dn * wide, -1, keepdims=True))
            dh_ref[...] = dh1_ref[...] + back.astype(bf16)

        @pl.when(i == steps - 1)
        def _():
            dw_ref[...] = dw_s[...].astype(bf16)

    queries = pl.BlockSpec((heads, tile, HEAD), lambda i: (0, i, 0))
    half = tiles(tile, HEAD // 2)
    return run(
        body, (steps,), [h, dq, dk, dv, cos, sin] + ([] if first else [dh1, qkvo]),
        [tiles(tile, d), queries, queries, queries, half, half] + ([] if first else [tiles(tile, d), whole(qkvo.shape)]),
        [sds((3, d, width), bf16)] + ([] if first else [sds((tokens, d), bf16)]),
        [whole((3, d, width))] + ([] if first else [tiles(tile, d)]),
        [pltpu.VMEM((3, d, width), f32)], side=side, ident=ident, flops=(6 if first else 12) * tokens * d * width, name="project_back")


def adamw(weights, m, v, gradients):
    arrays, at = [], {}
    for one in gradients:
        for array, _ in one:
            if id(array) not in at:
                at[id(array)] = len(arrays)
                arrays.append(array)
    count = len(weights)

    def kernel(*refs):
        w_refs, m_refs, v_refs = (refs[i * count : (i + 1) * count] for i in range(3))
        g_refs = refs[3 * count : 3 * count + len(arrays)]
        outs = refs[3 * count + len(arrays) :]
        for i in range(count):
            for number, (array, index) in enumerate(gradients[i]):
                g = g_refs[at[id(array)]][index].astype(f32)
                w = w_refs[i][number].astype(f32)
                new_m = 0.9 * m_refs[i][number] + 0.1 * g
                new_v = 0.95 * v_refs[i][number] + 0.05 * g * g
                step = new_m * lax.rsqrt(new_v + 1e-8) + 0.1 * w
                outs[i][number] = (w - 0.02 * step).astype(bf16)
                outs[count + i][number] = new_m
                outs[2 * count + i][number] = new_v

    return pl.pallas_call(
        kernel,
        in_specs=[VMEM] * (3 * count + len(arrays)),
        out_specs=[VMEM] * (3 * count),
        out_shape=[sds(w.shape, bf16) for w in weights] + [sds(w.shape, f32) for w in weights] * 2,
        compiler_params=pltpu.CompilerParams(vmem_limit_bytes=48 * MIB),
        name="adamw",
    )(*weights, *m, *v, *arrays)


def solution(mesh):
    devices = mesh.shape["dp"]

    def step(x, dy, *arrays):
        weights, m, v = (arrays[i : i + 7] for i in (0, 7, 14))
        layers = weights[0].shape[0]
        h = x[0]
        tokens, d = h.shape
        cos, sin = table(tokens)
        idents = iter(range(64))

        def alone(side):
            return run(None, (1,), [], [], [], [], side=side, ident=next(idents), name="ring")[1]

        def gather_small(number):
            full = sds((4, weights[0].shape[1] * devices, weights[0].shape[2]), bf16)
            return Gather(devices, weights[:4], number, [full], [(0, i) for i in range(4)])

        def gather_large(number):
            full = [sds((w.shape[1] * devices, w.shape[2]), bf16) for w in weights[4:]]
            return Gather(devices, weights[4:], number, full, [(i, None) for i in range(3)])

        def terms(g):
            m_ = g.shape[0] if g.ndim == 3 else 1
            return g.reshape(m_, devices // 2, 2, g.shape[-2] // devices, g.shape[-1])

        kept, full = [], []
        for number in range(layers):
            (qkvo,) = alone(gather_small(number))
            large = alone(gather_large(number))
            (q, k, vv), _ = project(h, qkvo, cos, sin)
            (o, lse), _ = attend(q, k, vv)
            (h1, gate, up, *rest), _ = feed(h, o, qkvo, *large, last=number == layers - 1)
            kept.append((h, q, k, vv, o, lse, h1, gate, up))
            full.append((qkvo, large))
            h = rest[0] if rest else None
        dh = dy[0]
        mine = [None] * layers
        for number in reversed(range(layers)):
            h, q, k, vv, o, lse, h1, gate, up = kept[number]
            qkvo, large = full[number]
            (dh1, dg, du, dd), _ = feed_back(h1, gate, up, dh, *large)
            big = alone(Scatter(devices, [terms(t) for t in (dg, du, dd)]))
            (do, delta, dwo), _ = out_back(dh1, o, qkvo, q.shape[0])
            (dq, dk, dv), _ = attend_back(q, k, vv, do, lse, delta)
            (dqkv, *rest), _ = project_back(h, dq, dk, dv, cos, sin, dh1, qkvo, number == 0)
            small = alone(Scatter(devices, [terms(dqkv), terms(dwo)]))
            mine[number] = [(small[0], 0), (small[0], 1), (small[0], 2), (small[1], 0), (big[0], 0), (big[1], 0), (big[2], 0)]
            dh = rest[0] if rest else None
        return tuple(adamw(weights, m, v, [[mine[number][i] for number in range(layers)] for i in range(7)]))

    states, cut = P(("rep", "dp"), None, None), P(None, "dp", None)
    return jax.shard_map(
        step,
        mesh=mesh,
        in_specs=(states, states) + (cut,) * 21,
        out_specs=(P("rep", "dp", None),) * 21,
        check_vma=False,
    )
```

```python
import functools

import jax
import jax.numpy as jnp
import numpy as np
from jax import lax
from jax.experimental import pallas as pl
from jax.experimental.pallas import tpu as pltpu
from jax.sharding import PartitionSpec as P

HEAD = 256
THETA = 10000
NAMES = ("wq", "wk", "wv", "wo", "w_gate", "w_up", "w_down")
LOG2E = 1.4426950408889634
NEG = -1e30
MIB = 2**20
MESH = pl.DeviceIdType.MESH
bf16, f32 = jnp.bfloat16, jnp.float32
ANY = pl.BlockSpec(memory_space=pl.ANY)
VMEM = pl.BlockSpec(memory_space=pltpu.VMEM)


def dot(a, b, ca=1, cb=0):
    return lax.dot_general(a, b, (((ca,), (cb,)), ((), ())), preferred_element_type=f32)


def sds(shape, dtype):
    return jax.ShapeDtypeStruct(shape, dtype)


class Place:
    def __init__(self, devices):
        me = lax.axis_index("dp")
        self.me, self.chips = me, devices // 2
        self.z, self.c = me // 2, lax.rem(me, 2)
        self.right = lax.rem(me + 2, devices)
        self.left = lax.rem(me + devices - 2, devices)
        self.partner = me + 1 - 2 * self.c

    def chip(self, away):
        return lax.rem(self.z + (away + self.chips), self.chips)


def hops(devices, flip):
    chips = devices // 2
    far, near = chips // 2, chips - 1 - chips // 2
    return (near, far) if flip else (far, near)


def meet(devices):
    p = Place(devices)
    barrier = pltpu.get_barrier_semaphore()
    for other in (p.left, p.right, p.partner):
        pl.semaphore_signal(barrier, inc=1, device_id={"dp": other}, device_id_type=MESH)
    pl.semaphore_wait(barrier, 3)


class Gather:
    def __init__(self, devices, shards, layer, outs, where):
        self.devices, self.layer, self.where = devices, layer, where
        self.ins = list(shards)
        self.in_specs = [
            pl.BlockSpec((1,) + s.shape[1:], lambda *_: (layer, 0, 0)) for s in shards
        ]
        self.outs = outs
        self.out_specs = [ANY] * len(outs)
        self.units = len(shards)
        slots = 2 * (devices // 2) + 1
        self.scratch = [
            pltpu.SemaphoreType.DMA((self.units, slots)),
            pltpu.SemaphoreType.DMA((self.units, slots)),
            pltpu.SemaphoreType.DMA((self.units,)),
        ]

    def bind(self, ins, outs, scratch):
        self.rows, self.full = ins, outs
        self.send, self.recv, self.local = scratch

    def view(self, u, device):
        out, index = self.where[u]
        r = self.ins[u].shape[1]
        rows = pl.ds(pl.multiple_of(device * r, r), r)
        return self.full[out].at[rows, :] if index is None else self.full[out].at[index, rows, :]

    def copy(self, u, slot, source, device, to):
        return pltpu.make_async_remote_copy(
            src_ref=source, dst_ref=self.view(u, device), send_sem=self.send.at[u, slot], recv_sem=self.recv.at[u, slot],
            device_id={"dp": to}, device_id_type=MESH)

    def flows(self, u):
        right, left = hops(self.devices, u % 2)
        half = self.devices // 4
        return (right, 0, 2 * half, 1), (left, half, 3 * half, -1)

    def first(self, u):
        p = Place(self.devices)
        own = self.rows[u].at[0]
        pltpu.make_async_copy(own, self.view(u, p.me), self.local.at[u]).start()
        (_, a, _, _), (_, b, _, _) = self.flows(u)
        self.copy(u, a, own, p.me, p.right).start()
        self.copy(u, b, own, p.me, p.left).start()
        self.copy(u, self.devices, own, p.me, p.partner).start()

    def hop(self, u, s):
        p = Place(self.devices)
        for count, ring, across, way in self.flows(u):
            if s > count:
                continue
            device = 2 * p.chip(-way * s) + p.c
            here = self.view(u, device)
            to = p.right if way == 1 else p.left
            self.copy(u, ring + s - 1, here, device, to).wait_recv()
            if s < count:
                self.copy(u, ring + s, here, device, to).start()
            self.copy(u, across + s - 1, here, device, p.partner).start()

    def last(self, u):
        p = Place(self.devices)
        own = self.rows[u].at[0]
        pltpu.make_async_copy(own, self.view(u, p.me), self.local.at[u]).wait()
        self.copy(u, self.devices, own, p.partner, p.partner).wait_recv()
        self.copy(u, self.devices, own, p.me, p.partner).wait_send()
        for count, ring, across, way in self.flows(u):
            to = p.right if way == 1 else p.left
            for s in range(1, count + 1):
                device = 2 * p.chip(-way * s) + p.c
                theirs = 2 * p.chip(-way * s) + 1 - p.c
                self.copy(u, across + s - 1, self.view(u, theirs), theirs, p.partner).wait_recv()
                self.copy(u, across + s - 1, self.view(u, device), device, p.partner).wait_send()
                self.copy(u, ring + s - 1, self.view(u, device), device, to).wait_send()

    def steps(self):
        most = max(hops(self.devices, 0))
        units = range(self.units)
        out = [functools.partial(self.first, u) for u in units]
        for s in range(1, most + 1):
            out += [functools.partial(self.hop, u, s) for u in units]
        return out, [functools.partial(self.last, u) for u in units]


class Scatter:
    def __init__(self, devices, terms):
        self.devices = devices
        self.ins = list(terms)
        self.in_specs = [ANY] * len(terms)
        self.units = len(terms)
        self.outs, self.out_specs, self.scratch = [], [], []
        chips = devices // 2
        for t in terms:
            m, _, _, r, n = t.shape
            self.outs.append(sds((m, r, n), bf16))
            self.out_specs.append(pl.BlockSpec((m, r, n), lambda *_: (0, 0, 0)))
            self.scratch += [
                pltpu.VMEM((m, chips, r, n), bf16),
                pltpu.VMEM((m, chips, r, n), bf16),
                pltpu.VMEM((chips, m, r, n), bf16),
                pltpu.VMEM((chips, m, r, n), bf16),
            ]
        self.scratch += [
            pltpu.SemaphoreType.DMA((self.units, chips + 1)),
            pltpu.SemaphoreType.DMA((self.units, chips + 1)),
            pltpu.SemaphoreType.DMA((self.units,)),
        ]

    def bind(self, ins, outs, scratch):
        self.terms, self.result = ins, outs
        self.own = scratch[0 : 4 * self.units : 4]
        self.pair = scratch[1 : 4 * self.units : 4]
        self.come = scratch[2 : 4 * self.units : 4]
        self.gone = scratch[3 : 4 * self.units : 4]
        self.send, self.recv, self.local = scratch[4 * self.units :]

    def flows(self, u):
        right, left = hops(self.devices, u % 2)
        return (right, 0, 1), (left, self.devices // 4, -1)

    def mine(self, u, p):
        return pltpu.make_async_copy(self.terms[u].at[:, :, p.c], self.own[u], self.local.at[u])

    def swap(self, u, p):
        slot = self.devices // 2
        return pltpu.make_async_remote_copy(
            src_ref=self.terms[u].at[:, :, 1 - p.c], dst_ref=self.pair[u], send_sem=self.send.at[u, slot], recv_sem=self.recv.at[u, slot],
            device_id={"dp": p.partner}, device_id_type=MESH)

    def copy(self, u, slot, to):
        return pltpu.make_async_remote_copy(
            src_ref=self.gone[u].at[slot], dst_ref=self.come[u].at[slot], send_sem=self.send.at[u, slot], recv_sem=self.recv.at[u, slot],
            device_id={"dp": to}, device_id_type=MESH)

    def first(self, u):
        p = Place(self.devices)
        self.mine(u, p).start()
        self.swap(u, p).start()

    def both(self, u, i, chip):
        return self.own[u][i, chip].astype(f32) + self.pair[u][i, chip].astype(f32)

    def hop(self, u, s):
        p = Place(self.devices)
        if s == 1:
            self.mine(u, p).wait()
            self.swap(u, p).wait_recv()
        for count, slot, way in self.flows(u):
            if s > count:
                continue
            to = p.right if way == 1 else p.left
            chip = p.chip(way * (count - s + 1))
            if s > 1:
                self.copy(u, slot + s - 2, to).wait_recv()
            for i in range(self.ins[u].shape[0]):
                total = self.both(u, i, chip)
                if s > 1:
                    total += self.come[u][slot + s - 2, i].astype(f32)
                self.gone[u][slot + s - 1, i] = total.astype(bf16)
            self.copy(u, slot + s - 1, to).start()

    def last(self, u):
        p = Place(self.devices)
        self.swap(u, p).wait_send()
        for count, slot, way in self.flows(u):
            to = p.right if way == 1 else p.left
            self.copy(u, slot + count - 1, to).wait_recv()
            for s in range(count):
                self.copy(u, slot + s, to).wait_send()
        for i in range(self.ins[u].shape[0]):
            total = self.both(u, i, p.z)
            for count, slot, _ in self.flows(u):
                total += self.come[u][slot + count - 1, i].astype(f32)
            self.result[u][i] = total.astype(bf16)

    def steps(self):
        most = max(hops(self.devices, 0))
        units = range(self.units)
        out = [functools.partial(self.first, u) for u in units]
        for s in range(1, most + 1):
            out += [functools.partial(self.hop, u, s) for u in units]
        return out, [functools.partial(self.last, u) for u in units]


def run(body, grid, ins, in_specs, outs, out_specs, scratch=(), side=None, ident=None, vmem=60, flops=0, name=None, pokes=1):
    counts = [len(ins), len(side.ins) if side else 0, len(outs), len(side.outs) if side else 0, len(scratch), len(side.scratch) if side else 0]
    places = grid * pokes

    def kernel(*refs):
        parts, at = [], 0
        for n in counts:
            parts.append(list(refs[at : at + n]))
            at += n
        step = pl.program_id(0)
        due, end = {}, []
        if side:
            side.bind(parts[1], parts[3], parts[5])
            todo, end = side.steps()
            for i, one in enumerate(todo):
                due.setdefault(i * places // len(todo), []).append(one)

        def poke(place):
            for at in sorted(due):
                if at % pokes == place:

                    @pl.when(step == at // pokes)
                    def _():
                        if at == 0:
                            meet(side.devices)
                        for one in due[at]:
                            one()

        poke(0)
        if body:
            body(poke, *parts[0], *parts[2], *parts[4])
        if side:

            @pl.when(step == grid - 1)
            def _():
                for one in end:
                    one()

    got = pl.pallas_call(
        kernel,
        grid=(grid,),
        in_specs=list(in_specs) + (side.in_specs if side else []),
        out_specs=list(out_specs) + (side.out_specs if side else []),
        out_shape=list(outs) + (side.outs if side else []),
        scratch_shapes=list(scratch) + (side.scratch if side else []),
        compiler_params=pltpu.CompilerParams(
            dimension_semantics=("arbitrary",), vmem_limit_bytes=int(vmem * MIB),
            **(dict(collective_id=ident, has_side_effects=True) if side else {})),
        cost_estimate=pl.CostEstimate(flops=flops, bytes_accessed=sum(a.size * a.dtype.itemsize for a in (*ins, *outs)), transcendentals=0),
        name=name,
    )(*ins, *(side.ins if side else []))
    return got[: len(outs)], got[len(outs) :]


def scale_of(wide):
    return lax.rsqrt(jnp.mean(wide * wide, -1, keepdims=True) + 1e-6)


def turn(t, cos, sin):
    half = t.shape[-1] // 2
    a, b = t[:, :half].astype(f32), t[:, half:].astype(f32)
    return jnp.concatenate([a * cos - b * sin, b * cos + a * sin], -1).astype(bf16)


def table(tokens):
    half = HEAD // 2
    angle = np.arange(tokens, dtype=np.float32)[:, None] * np.power(np.float32(THETA), -np.arange(half, dtype=np.float32) / np.float32(half))
    return jnp.asarray(np.cos(angle).astype(np.float32)), jnp.asarray(np.sin(angle).astype(np.float32))


def whole(shape):
    return pl.BlockSpec(shape, lambda *_: (0,) * len(shape))


def tiles(rows, columns):
    return pl.BlockSpec((rows, columns), lambda i, *_: (i, 0))


def look(h, qkvo, cos, sin, side=None, ident=None):
    tokens, d = h.shape
    heads = qkvo.shape[2] // HEAD
    b = 512
    e = HEAD**-0.5 * LOG2E

    def body(poke, h_ref, w_ref, cos_ref, sin_ref, q_ref, k_ref, v_ref, o_ref, lse_ref, k_s, v_s, top_s, mix_s):
        iq = pl.program_id(0)
        mine = pl.ds(pl.multiple_of(iq * b, b), b)
        wide = h_ref[...].astype(f32)
        a = (wide * scale_of(wide)).astype(bf16)
        for i, (out, all_s) in enumerate(((q_ref, None), (k_ref, k_s), (v_ref, v_s))):
            t = dot(a, w_ref[i]).astype(bf16)
            for n in range(heads):
                one = t[:, n * HEAD : (n + 1) * HEAD]
                one = one if i == 2 else turn(one, cos_ref[...], sin_ref[...])
                out[n] = one
                if i:
                    all_s[n, mine, :] = one
        poke(1)
        top_s[...] = jnp.full(top_s.shape, NEG, f32)
        mix_s[...] = jnp.zeros(mix_s.shape, f32)
        ones = jnp.ones((8, b), bf16)

        def block(j, masked):
            here = pl.ds(pl.multiple_of(j * b, b), b)
            scores = [dot(k_s[n, here, :], q_ref[n], 1, 1) for n in range(heads)]
            weights, keeps = [], []
            for n, s in enumerate(scores):
                if masked:
                    seen = lax.broadcasted_iota(jnp.int32, (b, b), 0) <= lax.broadcasted_iota(jnp.int32, (b, b), 1)
                    s = jnp.where(seen, s, 2 * NEG)
                old = top_s[n : n + 1, :]
                top = jnp.maximum(old, s.max(axis=0, keepdims=True))
                top_s[n : n + 1, :] = top
                weights.append(jnp.exp2((s - top) * e).astype(bf16))
                keeps.append(jnp.exp2((old - top) * e))
            for n in range(heads):
                values = jnp.concatenate([v_s[n, here, :].T, ones], axis=0)
                mix_s[n] = mix_s[n] * keeps[n] + dot(values, weights[n])

        lax.fori_loop(0, iq, lambda j, _: block(j, False), None)
        poke(2)
        block(iq, True)
        for n in range(heads):
            total = mix_s[n, HEAD : HEAD + 1, :]
            o_ref[:, n * HEAD : (n + 1) * HEAD] = (mix_s[n, :HEAD, :] * (1 / total)).T.astype(bf16)
            lse_ref[n : n + 1, :] = top_s[n : n + 1, :] * HEAD**-0.5 + jnp.log(total)

    out = pl.BlockSpec((heads, b, HEAD), lambda i: (0, i, 0))
    return run(
        body, tokens // b, [h, qkvo, cos, sin],
        [tiles(b, d), whole(qkvo.shape), tiles(b, HEAD // 2), tiles(b, HEAD // 2)],
        [sds((heads, tokens, HEAD), bf16)] * 3 + [sds((tokens, heads * HEAD), bf16), sds((heads, tokens), f32)],
        [out] * 3 + [tiles(b, heads * HEAD), pl.BlockSpec((heads, b), lambda i: (0, i))],
        [pltpu.VMEM((heads, tokens, HEAD), bf16)] * 2 + [pltpu.VMEM((heads, b), f32), pltpu.VMEM((heads, HEAD + 8, b), f32)],
        side=side, ident=ident, flops=6 * tokens * d * heads * HEAD + 2 * heads * tokens * tokens * HEAD, name="look", pokes=3)


def feed(h, o, qkvo, gate_w, up_w, down_w, last, side=None, ident=None):
    tokens, d = h.shape
    ff = gate_w.shape[1]
    tile, part = 512, 512

    def body(poke, h_ref, o_ref, wo_ref, g_ref, u_ref, d_ref, h1_ref, gate_ref, up_ref, *rest):
        h1 = h_ref[...] + dot(o_ref[...], wo_ref[0]).astype(bf16)
        h1_ref[...] = h1
        wide = h1.astype(f32)
        b = (wide * scale_of(wide)).astype(bf16)
        total = None
        for at in range(0, ff, part):
            if at:
                poke(at // part)
            gate = dot(b, g_ref[:, at : at + part])
            up = dot(b, u_ref[:, at : at + part])
            gate_ref[:, at : at + part] = gate
            up_ref[:, at : at + part] = up
            if rest:
                p = (gate * jax.nn.sigmoid(gate) * up).astype(bf16)
                one = dot(p, d_ref[at : at + part, :])
                total = one if total is None else total + one
        if rest:
            rest[0][...] = h1 + total.astype(bf16)

    once = lambda shape: pl.BlockSpec(shape, lambda i: (0,) * len(shape), pipeline_mode=pl.Buffered(1))
    rows = tiles(tile, d)
    return run(
        body, tokens // tile, [h, o, qkvo, gate_w, up_w, down_w],
        [rows, tiles(tile, o.shape[1]), pl.BlockSpec((1,) + qkvo.shape[1:], lambda i: (3, 0, 0)), once(gate_w.shape), once(up_w.shape), once(down_w.shape)],
        [sds((tokens, d), bf16), sds((tokens, ff), f32), sds((tokens, ff), f32)] + ([] if last else [sds((tokens, d), bf16)]),
        [rows, tiles(tile, ff), tiles(tile, ff)] + ([] if last else [rows]),
        side=side, ident=ident, flops=2 * tokens * d * (d + 3 * ff), name="feed", pokes=ff // part)


def feed_back(h1, gate, up, dh2, gate_w, up_w, down_w, side=None, ident=None):
    tokens, d = h1.shape
    ff = gate.shape[1]
    part, tile = 256, 512
    steps = ff // part

    def body(poke, h1_ref, gate_ref, up_ref, dh2_ref, g_ref, u_ref, d_ref, dh1_ref, dg_ref, du_ref, dd_ref, b_s, p_s, dgate_s, dup_s, db_s):
        f = pl.program_id(0)

        @pl.when(f == 0)
        def _():
            for t in range(0, tokens, tile):
                wide = h1_ref[t : t + tile, :].astype(f32)
                b_s[t : t + tile, :] = (wide * scale_of(wide)).astype(bf16)
                db_s[t : t + tile, :] = jnp.zeros((tile, d), f32)

        for t in range(0, tokens, tile):
            here = slice(t, t + tile)
            dp = dot(dh2_ref[here, :], d_ref[...], 1, 1).astype(bf16).astype(f32)
            gate, up = gate_ref[here, :], up_ref[here, :]
            s = jax.nn.sigmoid(gate)
            soft = gate * s
            p_s[here, :] = (soft * up).astype(bf16)
            dup = (dp * soft).astype(bf16)
            dgate = (dp * up * (s + soft * (1 - s))).astype(bf16)
            dup_s[here, :] = dup
            dgate_s[here, :] = dgate
            db_s[here, :] += dot(dgate, g_ref[...], 1, 1) + dot(dup, u_ref[...], 1, 1)
        poke(1)
        dd_ref[...] = dot(p_s[...], dh2_ref[...], 0, 0).astype(bf16)
        dg_ref[...] = dot(b_s[...], dgate_s[...], 0, 0).astype(bf16)
        du_ref[...] = dot(b_s[...], dup_s[...], 0, 0).astype(bf16)

        @pl.when(f == steps - 1)
        def _():
            for t in range(0, tokens, tile):
                here = slice(t, t + tile)
                wide = h1_ref[here, :].astype(f32)
                dn = db_s[here, :].astype(bf16).astype(f32)
                scale = scale_of(wide)
                back = scale * dn - wide * (scale * scale * scale * jnp.mean(dn * wide, -1, keepdims=True))
                dh1_ref[here, :] = dh2_ref[here, :] + back.astype(bf16)

    columns = lambda rows: pl.BlockSpec((rows, part), lambda f: (0, f))
    down = pl.BlockSpec((part, d), lambda f: (f, 0))
    return run(
        body, steps, [h1, gate, up, dh2, gate_w, up_w, down_w],
        [whole((tokens, d)), columns(tokens), columns(tokens), whole((tokens, d)), columns(d), columns(d), down],
        [sds((tokens, d), bf16), sds((d, ff), bf16), sds((d, ff), bf16), sds((ff, d), bf16)],
        [whole((tokens, d)), columns(d), columns(d), down],
        [pltpu.VMEM((tokens, d), bf16)] + [pltpu.VMEM((tokens, part), bf16)] * 3 + [pltpu.VMEM((tokens, d), f32)],
        side=side, ident=ident, flops=12 * tokens * d * ff, name="feed_back", pokes=2)


def look_back(h, q, k, v, o, lse, dh1, qkvo, cos, sin, first, side=None, ident=None):
    tokens, d = h.shape
    heads = q.shape[0]
    width = heads * HEAD
    b = 512
    scale = HEAD**-0.5
    e = scale * LOG2E
    half = tokens // b

    def body(poke, h_ref, q_ref, k_ref, v_ref, o_ref, lse_ref, dh1_ref, w_ref, cos_ref, sin_ref, *rest):
        dwo_ref, dw_ref, *rest = rest
        dh_ref = None if first else rest[0]
        dq_a, dk_s, dv_s, dq_s, do_s, dwo_s, dw_s = rest[0 if first else 1 :]
        i = pl.program_id(0)

        @pl.when(i == 0)
        def _():
            dk_s[...] = jnp.zeros(dk_s.shape, f32)
            dv_s[...] = jnp.zeros(dv_s.shape, f32)
            dwo_s[...] = jnp.zeros(dwo_s.shape, f32)
            dw_s[...] = jnp.zeros(dw_s.shape, f32)

        @pl.when(i < half)
        def _():
            mine = pl.ds(pl.multiple_of(i * b, b), b)
            do_s[...] = dot(dh1_ref[...], w_ref[3], 1, 1).astype(bf16)
            dwo_s[...] += dot(o_ref[...], dh1_ref[...], 0, 0)
            deltas = []
            for n in range(heads):
                cut = slice(n * HEAD, (n + 1) * HEAD)
                deltas.append((do_s[:, cut].astype(f32) * o_ref[:, cut].astype(f32)).T.sum(axis=0, keepdims=True))
            dq_s[...] = jnp.zeros(dq_s.shape, f32)

            def block(j, masked):
                here = pl.ds(pl.multiple_of(j * b, b), b)
                dos = [do_s[:, n * HEAD : (n + 1) * HEAD] for n in range(heads)]
                scores = [dot(k_ref[n, here, :], q_ref[n], 1, 1) for n in range(heads)]
                dps = [dot(v_ref[n, here, :], dos[n], 1, 1) for n in range(heads)]
                for n in range(heads):
                    p = jnp.exp2(scores[n] * e - lse_ref[n : n + 1, :] * LOG2E)
                    if masked:
                        seen = lax.broadcasted_iota(jnp.int32, (b, b), 0) <= lax.broadcasted_iota(jnp.int32, (b, b), 1)
                        p = jnp.where(seen, p, 0.0)
                    ds = (p * (dps[n] - deltas[n])).astype(bf16)
                    dv_s[n, here, :] += dot(p.astype(bf16), dos[n])
                    dk_s[n, here, :] += dot(ds, q_ref[n])
                    dq_s[n] += dot(k_ref[n, here, :].T, ds)

            lax.fori_loop(0, i, lambda j, _: block(j, False), None)
            block(i, True)
            for n in range(heads):
                dq_a[n, mine, :] = (dq_s[n] * scale).T.astype(bf16)

        poke(1)

        @pl.when(i >= half)
        def _():
            mine = pl.ds(pl.multiple_of((i - half) * b, b), b)
            wide = h_ref[...].astype(f32)
            size = scale_of(wide)
            a = (wide * size).astype(bf16)
            back = None
            for n in range(3):
                if n == 0:
                    some = [turn(dq_a[m, mine, :], cos_ref[...], -sin_ref[...]) for m in range(heads)]
                elif n == 1:
                    some = [turn((dk_s[m, mine, :] * scale).astype(bf16), cos_ref[...], -sin_ref[...]) for m in range(heads)]
                else:
                    some = [dv_s[m, mine, :].astype(bf16) for m in range(heads)]
                t = jnp.concatenate(some, axis=1)
                dw_s[n] += dot(a, t, 0, 0)
                if not first:
                    part = dot(t, w_ref[n], 1, 1)
                    back = part if back is None else back + part
            if not first:
                dn = back.astype(bf16).astype(f32)
                back = size * dn - wide * (size * size * size * jnp.mean(dn * wide, -1, keepdims=True))
                dh_ref[...] = dh1_ref[...] + back.astype(bf16)

        @pl.when(i == 2 * half - 1)
        def _():
            dwo_ref[...] = dwo_s[...].astype(bf16)
            dw_ref[...] = dw_s[...].astype(bf16)

    early = lambda i: jnp.minimum(i, half - 1)
    late = lambda i: jnp.maximum(i - half, 0)
    return run(
        body, 2 * half, [h, q, k, v, o, lse, dh1, qkvo, cos, sin],
        [pl.BlockSpec((b, d), lambda i: (late(i), 0)), pl.BlockSpec((heads, b, HEAD), lambda i: (0, early(i), 0)),
         whole((heads, tokens, HEAD)), whole((heads, tokens, HEAD)), pl.BlockSpec((b, width), lambda i: (early(i), 0)),
         pl.BlockSpec((heads, b), lambda i: (0, early(i))), pl.BlockSpec((b, d), lambda i: (lax.rem(i, half), 0)), whole(qkvo.shape),
         pl.BlockSpec((b, HEAD // 2), lambda i: (late(i), 0)), pl.BlockSpec((b, HEAD // 2), lambda i: (late(i), 0))],
        [sds((width, d), bf16), sds((3, d, width), bf16)] + ([] if first else [sds((tokens, d), bf16)]),
        [whole((width, d)), whole((3, d, width))] + ([] if first else [pl.BlockSpec((b, d), lambda i: (late(i), 0))]),
        [pltpu.VMEM((heads, tokens, HEAD), bf16), pltpu.VMEM((heads, tokens, HEAD), f32), pltpu.VMEM((heads, tokens, HEAD), f32),
         pltpu.VMEM((heads, HEAD, b), f32), pltpu.VMEM((b, width), bf16), pltpu.VMEM((width, d), f32), pltpu.VMEM((3, d, width), f32)],
        side=side, ident=ident, flops=5 * heads * tokens * tokens * HEAD + (10 if first else 16) * tokens * d * width, name="look_back", pokes=2)


def adamw(weights, m, v, gradients):
    arrays, at = [], {}
    for one in gradients:
        for array, _ in one:
            if id(array) not in at:
                at[id(array)] = len(arrays)
                arrays.append(array)
    count = len(weights)

    def kernel(*refs):
        w_refs, m_refs, v_refs = (refs[i * count : (i + 1) * count] for i in range(3))
        g_refs = refs[3 * count : 3 * count + len(arrays)]
        outs = refs[3 * count + len(arrays) :]
        for i in range(count):
            for number, (array, index) in enumerate(gradients[i]):
                g = g_refs[at[id(array)]][index].astype(f32)
                w = w_refs[i][number].astype(f32)
                new_m = 0.9 * m_refs[i][number] + 0.1 * g
                new_v = 0.95 * v_refs[i][number] + 0.05 * g * g
                step = new_m * lax.rsqrt(new_v + 1e-8) + 0.1 * w
                outs[i][number] = (w - 0.02 * step).astype(bf16)
                outs[count + i][number] = new_m
                outs[2 * count + i][number] = new_v

    return pl.pallas_call(
        kernel,
        in_specs=[VMEM] * (3 * count + len(arrays)),
        out_specs=[VMEM] * (3 * count),
        out_shape=[sds(w.shape, bf16) for w in weights] + [sds(w.shape, f32) for w in weights] * 2,
        compiler_params=pltpu.CompilerParams(vmem_limit_bytes=63 * MIB),
        name="adamw",
    )(*weights, *m, *v, *arrays)


def solution(mesh):
    devices = mesh.shape["dp"]

    def step(x, dy, *arrays):
        weights, m, v = (arrays[i : i + 7] for i in (0, 7, 14))
        layers = weights[0].shape[0]
        h = x[0]
        tokens, d = h.shape
        cos, sin = table(tokens)
        idents = iter(range(64))

        def alone(side):
            return run(None, 1, [], [], [], [], side=side, ident=next(idents), name="ring")[1]

        def gather_small(number):
            full = sds((4, weights[0].shape[1] * devices, weights[0].shape[2]), bf16)
            return Gather(devices, weights[:4], number, [full], [(0, i) for i in range(4)])

        def gather_large(number):
            full = [sds((w.shape[1] * devices, w.shape[2]), bf16) for w in weights[4:]]
            return Gather(devices, weights[4:], number, full, [(i, None) for i in range(3)])

        def terms(g):
            m_ = g.shape[0] if g.ndim == 3 else 1
            return g.reshape(m_, devices // 2, 2, g.shape[-2] // devices, g.shape[-1])

        kept, full = [], []
        (qkvo,) = alone(gather_small(0))
        for number in range(layers):
            last = number == layers - 1
            (q, k, vv, o, lse), large = look(h, qkvo, cos, sin, side=gather_large(number), ident=next(idents))
            more = {} if last else dict(side=gather_small(number + 1), ident=next(idents))
            (h1, gate, up, *rest), coming = feed(h, o, qkvo, *large, last, **more)
            kept.append((h, q, k, vv, o, lse, h1, gate, up))
            full.append((qkvo, large))
            if not last:
                (h,), (qkvo,) = rest, coming
        dh, small = dy[0], None
        mine = [[None] * 7 for _ in range(layers)]

        def got_small(number, some):
            mine[number][:4] = [(some[0], 0), (some[0], 1), (some[0], 2), (some[1], 0)]

        for number in reversed(range(layers)):
            h, q, k, vv, o, lse, h1, gate, up = kept[number]
            qkvo, large = full[number]
            more = {} if small is None else dict(side=small, ident=next(idents))
            (dh1, dg, du, dd), done = feed_back(h1, gate, up, dh, *large, **more)
            if small is not None:
                got_small(number + 1, done)
            big = Scatter(devices, [terms(t) for t in (dg, du, dd)])
            (dwo, dqkv, *rest), done = look_back(h, q, k, vv, o, lse, dh1, qkvo, cos, sin, number == 0, side=big, ident=next(idents))
            mine[number][4:] = [(one, 0) for one in done]
            small = Scatter(devices, [terms(dqkv), terms(dwo)])
            dh = rest[0] if rest else None
        got_small(0, alone(small))
        return tuple(adamw(weights, m, v, [[mine[number][i] for number in range(layers)] for i in range(7)]))

    states, cut = P(("rep", "dp"), None, None), P(None, "dp", None)
    return jax.shard_map(
        step,
        mesh=mesh,
        in_specs=(states, states) + (cut,) * 21,
        out_specs=(P("rep", "dp", None),) * 21,
        check_vma=False,
    )
```

```python
import functools

import jax
import jax.numpy as jnp
import numpy as np
from jax import lax
from jax.experimental import pallas as pl
from jax.experimental.pallas import tpu as pltpu
from jax.sharding import PartitionSpec as P

HEAD = 256
THETA = 10000
NAMES = ("wq", "wk", "wv", "wo", "w_gate", "w_up", "w_down")
LOG2E = 1.4426950408889634
NEG = -1e30
MIB = 2**20
MESH = pl.DeviceIdType.MESH
bf16, f32 = jnp.bfloat16, jnp.float32
ANY = pl.BlockSpec(memory_space=pl.ANY)
VMEM = pl.BlockSpec(memory_space=pltpu.VMEM)


def dot(a, b, ca=1, cb=0):
    return lax.dot_general(a, b, (((ca,), (cb,)), ((), ())), preferred_element_type=f32)


def sds(shape, dtype):
    return jax.ShapeDtypeStruct(shape, dtype)


class Place:
    def __init__(self, groups, devices):
        me = lax.axis_index("dp")
        self.me, self.chips = me, devices // 2
        self.z, self.c = me // 2, lax.rem(me, 2)
        self.right = dict(dp=lax.rem(me + 2, devices))
        self.left = dict(dp=lax.rem(me + devices - 2, devices))
        self.partner = dict(dp=me + 1 - 2 * self.c)
        group, side = lax.axis_index("rep"), round(groups**0.5)
        x, y = group // side, lax.rem(group, side)
        self.beside = dict(rep=group + 1 - 2 * lax.rem(y, 2))
        self.above = dict(rep=group + side - 2 * side * lax.rem(x, 2))
        self.colour = lax.rem(x + y, 2)

    def chip(self, away):
        return lax.rem(self.z + (away + self.chips), self.chips)


def hops(devices, flip):
    chips = devices // 2
    far, near = chips // 2, chips - 1 - chips // 2
    return (near, far) if flip else (far, near)


def remote(source, target, send, recv, to):
    return pltpu.make_async_remote_copy(src_ref=source, dst_ref=target, send_sem=send, recv_sem=recv, device_id=to, device_id_type=MESH)


class Layout:
    def __init__(self, weights):
        by_name = dict(zip(NAMES, weights))
        self.width, self.at, self.rows = weights[0].shape[2], {}, 0
        for name in ("wq", "wk", "wv", "wo", "w_down", "w_gate", "w_up"):
            _, r, n = by_name[name].shape
            self.at[name] = (self.rows, r, n // self.width)
            self.rows += r * (n // self.width)

    def span(self, first, last=None):
        start, (end, r, pieces) = self.at[first][0], self.at[last or first]
        return start, end + r * pieces


class Gather:
    aliases = {}

    def __init__(self, groups, devices, weights, units):
        self.groups, self.devices, self.units = groups, devices, units
        self.layout, self.layers = Layout(weights), weights[0].shape[0]
        self.most = max(hops(devices, 0))
        chips = devices // 2
        self.outs = [sds((chips, 2, self.layout.rows, self.layout.width), bf16)] * self.layers
        self.out_specs = [ANY] * self.layers
        self.ins, self.in_specs = list(weights), [whole(w.shape) for w in weights]
        self.then = None
        slots = 3 * chips + 3
        self.scratch = [
            pltpu.VMEM((self.layers, self.layout.rows, self.layout.width), bf16),
            pltpu.SemaphoreType.DMA((len(units), slots)),
            pltpu.SemaphoreType.DMA((len(units), slots)),
            pltpu.SemaphoreType.DMA((len(units),)),
        ]

    def bind(self, ins, outs, scratch):
        self.shards, self.full = ins, outs
        self.pack, self.send, self.recv, self.local = scratch

    def meet(self):
        for name, ref in zip(NAMES, self.shards):
            at, r, pieces = self.layout.at[name]
            for n in range(pieces):
                self.pack[:, at + n * r : at + (n + 1) * r, :] = ref[:, :, n * self.layout.width : (n + 1) * self.layout.width]
        p = Place(self.groups, self.devices)
        greet(p.left, p.right, p.partner, p.beside, p.above)

    def rows(self, u, part):
        first, end = self.units[u]["span"]
        pieces, number = part
        n = (end - first) // pieces
        return pl.ds(first, n) if pieces == 1 else pl.ds(pl.multiple_of(first + number * n, 8), n)

    def half(self, u, p):
        return (2, p.colour) if self.units[u]["share"] else (1, 0)

    def flows(self, u, p):
        right, left = hops(self.devices, u % 2)
        return (right, 0, 1, p.right), (left, self.devices // 4, -1, p.left)

    def hand(self, u, slot, part, to, p):
        view = self.full[self.units[u]["layer"]].at[:, p.c, self.rows(u, part), :]
        return remote(view, view, self.send.at[u, slot], self.recv.at[u, slot], to)

    def hear(self, u, slot, part, to, p, core):
        view = self.full[self.units[u]["layer"]].at[:, core, self.rows(u, part), :]
        return remote(view, view, self.send.at[u, slot], self.recv.at[u, slot], to)

    def pass_on(self, u, s, count, slot, way, to, p):
        rows = self.rows(u, self.half(u, p))
        target = self.full[self.units[u]["layer"]].at[p.chip(-way * s), p.c, rows, :]
        source = self.pack.at[self.units[u]["layer"], rows, :] if s == 0 else target
        return remote(source, target, self.send.at[u, slot + s], self.recv.at[u, slot + s], to)

    def fine(self, u):
        return self.units[u]["share"] == "fine"

    def quarters(self, u, p, theirs=False):
        n = p.chips
        k = 1 - p.colour if theirs else p.colour
        for count, slot, way, _ in self.flows(u, p):
            for s in range(1, count + 1):
                copies = []
                for i, to in enumerate((p.beside, p.above)):
                    view = self.full[self.units[u]["layer"]].at[p.chip(-way * s), p.c, self.rows(u, (4, 2 * k + i)), :]
                    at = n + 3 + i * n + slot + s - 1
                    copies.append(remote(view, view, self.send.at[u, at], self.recv.at[u, at], to))
                yield s, copies

    def keep(self, u, p):
        rows = self.rows(u, (1, 0) if self.fine(u) else self.half(u, p))
        return pltpu.make_async_copy(self.pack.at[self.units[u]["layer"], rows, :], self.full[self.units[u]["layer"]].at[p.z, p.c, rows, :], self.local.at[u])

    def ring(self, u, s):
        p = Place(self.groups, self.devices)
        if s == 0:
            self.keep(u, p).start()
        for count, slot, way, to in self.flows(u, p):
            if 0 < s <= count:
                view = self.full[self.units[u]["layer"]].at[p.chip(-way * s), p.c, self.rows(u, self.half(u, p)), :]
                remote(view, view, self.send.at[u, slot + s - 1], self.recv.at[u, slot + s - 1], to).wait_recv()
            if s < count:
                self.pass_on(u, s, count, slot, way, to, p).start()
        if self.fine(u):
            for hop, copies in self.quarters(u, p):
                if hop == s:
                    for copy in copies:
                        copy.start()
        if s == self.most:
            self.keep(u, p).wait()
            for count, slot, way, to in self.flows(u, p):
                for t in range(count):
                    self.pass_on(u, t, count, slot, way, to, p).wait_send()

    def across(self, u, stage):
        p = Place(self.groups, self.devices)
        n, k = p.chips, p.colour
        share = self.units[u]["share"]
        if stage == 0 and share:
            self.hand(u, n, (4, 2 * k), p.beside, p).start()
            self.hand(u, n + 1, (4, 2 * k + 1), p.above, p).start()
        if stage == 1:
            if self.fine(u):
                for _, copies in self.quarters(u, p, theirs=True):
                    for copy in copies:
                        copy.wait_recv()
            elif share:
                self.hear(u, n, (4, 2 - 2 * k), p.beside, p, p.c).wait_recv()
                self.hear(u, n + 1, (4, 3 - 2 * k), p.above, p, p.c).wait_recv()
            self.hand(u, n + 2, (1, 0), p.partner, p).start()
        if stage == 2:
            self.hear(u, n + 2, (1, 0), p.partner, p, 1 - p.c).wait_recv()
            self.hand(u, n + 2, (1, 0), p.partner, p).wait_send()
            if self.fine(u):
                for _, copies in self.quarters(u, p):
                    for copy in copies:
                        copy.wait_send()
            elif share:
                self.hand(u, n, (4, 2 * k), p.beside, p).wait_send()
                self.hand(u, n + 1, (4, 2 * k + 1), p.above, p).wait_send()
            if self.then:
                self.then(u)

    def steps(self):
        out = []
        for u, unit in enumerate(self.units):
            todo = [functools.partial(self.ring, u, s) for s in range(self.most + 1)]
            todo += [functools.partial(self.across, u, stage) for stage in range(0 if unit["share"] is True else 1, 3)]
            out += zip(unit["at"], todo, strict=True)
        return sorted(out, key=lambda one: one[0])


def greet(*others):
    barrier = pltpu.get_barrier_semaphore()
    for other in others:
        pl.semaphore_signal(barrier, inc=1, device_id=other, device_id_type=MESH)
    pl.semaphore_wait(barrier, len(others))


class Scatter:
    aliases = {}

    def __init__(self, groups, devices, units):
        self.groups, self.devices, self.spec = groups, devices, units
        self.units = len(units)
        self.given = [u for u in range(self.units) if hasattr(units[u][0], "dtype")]
        self.ins = [units[u][0] for u in self.given]
        self.in_specs = [ANY] * len(self.ins)
        self.sources = [tuple(getattr(unit[0], "shape", unit[0])) for unit in units]
        self.outs, self.out_specs, self.scratch = [], [], []
        for u, (m, chips, _, r, _) in enumerate(self.sources):
            n = self.width(u)
            self.outs.append(sds((m, r, n), bf16))
            self.out_specs.append(pl.BlockSpec((m, r, n), lambda *_: (0, 0, 0)))
            self.scratch += [
                pltpu.VMEM((m, chips, r, n) if u in self.given else self.sources[u], bf16),
                pltpu.VMEM((m, chips, r, n), bf16),
                pltpu.VMEM((chips, m, r, n), bf16),
                pltpu.VMEM((chips, m, r, n), bf16),
            ]
        slots = devices // 2 + 1
        self.scratch += [
            pltpu.SemaphoreType.DMA((self.units, slots)),
            pltpu.SemaphoreType.DMA((self.units, slots)),
            pltpu.SemaphoreType.DMA((self.units,)),
        ]

    def width(self, u):
        first, end = self.spec[u][1]
        return end - first

    def columns(self, u):
        return pl.ds(self.spec[u][1][0], self.width(u))

    def bind(self, ins, outs, scratch):
        self.result = outs
        self.own = scratch[0 : 4 * self.units : 4]
        self.pair = scratch[1 : 4 * self.units : 4]
        self.come = scratch[2 : 4 * self.units : 4]
        self.gone = scratch[3 : 4 * self.units : 4]
        self.terms = {**dict(zip(self.given, ins)), **{u: self.own[u] for u in range(self.units) if u not in self.given}}
        self.send, self.recv, self.local = scratch[4 * self.units :]

    def meet(self):
        p = Place(self.groups, self.devices)
        greet(p.left, p.right, p.partner)

    def term(self, u):
        return self.own[u]

    def flows(self, u, p):
        right, left = hops(self.devices, u % 2)
        return (right, 0, 1, p.right), (left, self.devices // 4, -1, p.left)

    def mine(self, u, p):
        return pltpu.make_async_copy(self.terms[u].at[:, :, p.c, :, self.columns(u)], self.own[u], self.local.at[u])

    def swap(self, u, p):
        slot = self.devices // 2
        return remote(self.terms[u].at[:, :, 1 - p.c, :, self.columns(u)], self.pair[u], self.send.at[u, slot], self.recv.at[u, slot], p.partner)

    def copy(self, u, slot, to):
        return remote(self.gone[u].at[slot], self.come[u].at[slot], self.send.at[u, slot], self.recv.at[u, slot], to)

    def first(self, u):
        p = Place(self.groups, self.devices)
        if u in self.given:
            self.mine(u, p).start()
        self.swap(u, p).start()

    def both(self, u, i, chip, p):
        own = self.own[u][i, chip] if u in self.given else self.own[u][i, chip, p.c, :, self.columns(u)]
        return own.astype(f32) + self.pair[u][i, chip].astype(f32)

    def hop(self, u, s):
        p = Place(self.groups, self.devices)
        if s == 1:
            if u in self.given:
                self.mine(u, p).wait()
            self.swap(u, p).wait_recv()
        for count, slot, way, to in self.flows(u, p):
            if s > count:
                continue
            chip = p.chip(way * (count - s + 1))
            if s > 1:
                self.copy(u, slot + s - 2, to).wait_recv()
            for i in range(self.sources[u][0]):
                total = self.both(u, i, chip, p)
                if s > 1:
                    total += self.come[u][slot + s - 2, i].astype(f32)
                self.gone[u][slot + s - 1, i] = total.astype(bf16)
            self.copy(u, slot + s - 1, to).start()

    def last(self, u):
        p = Place(self.groups, self.devices)
        self.swap(u, p).wait_send()
        for count, slot, _, to in self.flows(u, p):
            self.copy(u, slot + count - 1, to).wait_recv()
        for i in range(self.sources[u][0]):
            total = self.both(u, i, p.z, p)
            for count, slot, _, _ in self.flows(u, p):
                total += self.come[u][slot + count - 1, i].astype(f32)
            self.result[u][i] = total.astype(bf16)
        for count, slot, _, to in self.flows(u, p):
            for s in range(count):
                self.copy(u, slot + s, to).wait_send()

    def steps(self):
        most = max(hops(self.devices, 0))
        out = []
        for u, (_, _, at) in enumerate(self.spec):
            out.append((at[0], functools.partial(self.first, u)))
            out += [(at[s], functools.partial(self.hop, u, s)) for s in range(1, most + 1)]
            out.append((at[most + 1], functools.partial(self.last, u)))
        return sorted(out, key=lambda one: one[0])


def run(body, grid, ins, in_specs, outs, out_specs, scratch=(), side=None, ident=None, vmem=60, flops=0, name=None, slots=1, prepare=None):
    counts = [len(ins), len(side.ins) if side else 0, len(outs), len(side.outs) if side else 0, len(scratch), len(side.scratch) if side else 0]

    def kernel(*refs):
        parts, at = [], 0
        for n in counts:
            parts.append(list(refs[at : at + n]))
            at += n
        due, early, end = {}, [], []
        if side:
            side.bind(parts[1], parts[3], parts[5])
            if prepare:
                prepare(*parts[4])
            for when, one in side.steps():
                slot = int(np.ceil(when - 1e-6))
                if when < 0:
                    early.append(one)
                elif slot < slots:
                    due.setdefault(slot, []).append(one)
                else:
                    end.append(one)

            @pl.when(pl.program_id(0) == 0)
            def _():
                side.meet()
                for one in early:
                    one()

        def poke(number, among):
            for at in among:
                if at in due:

                    @pl.when(number == at)
                    def _():
                        for one in due[at]:
                            one()

        if body:
            body(poke, *parts[0], *parts[2], *parts[4])
        if end:

            @pl.when(pl.program_id(0) == grid - 1)
            def _():
                for one in end:
                    one()

    got = pl.pallas_call(
        kernel,
        grid=(grid,),
        in_specs=list(in_specs) + (side.in_specs if side else []),
        out_specs=list(out_specs) + (side.out_specs if side else []),
        out_shape=list(outs) + (side.outs if side else []),
        scratch_shapes=list(scratch) + (side.scratch if side else []),
        input_output_aliases={len(ins) + i: len(outs) + o for i, o in side.aliases.items()} if side else {},
        compiler_params=pltpu.CompilerParams(
            dimension_semantics=("arbitrary",), vmem_limit_bytes=int(vmem * MIB),
            **(dict(collective_id=ident, has_side_effects=True) if side else {})),
        cost_estimate=pl.CostEstimate(flops=flops, bytes_accessed=sum(a.size * a.dtype.itemsize for a in (*ins, *outs)), transcendentals=0),
        name=name,
    )(*ins, *(side.ins if side else []))
    return got[: len(outs)], got[len(outs) :]


TILE = 512
FINE = 64


def scale_of(wide):
    return lax.rsqrt(jnp.mean(wide * wide, -1, keepdims=True) + 1e-6)


def turn(t, cos, sin):
    half = t.shape[-1] // 2
    a, b = t[:, :half].astype(f32), t[:, half:].astype(f32)
    return jnp.concatenate([a * cos - b * sin, b * cos + a * sin], -1).astype(bf16)


def table(tokens):
    half = HEAD // 2
    rate = np.float64(THETA) ** (-np.arange(half) / half)
    coarse, fine = (np.arange(n)[:, None] * step * rate for n, step in ((tokens // FINE, FINE), (FINE, 1)))
    return [jnp.asarray(np.stack([np.cos(a), np.sin(a)]).astype(np.float32)) for a in (coarse, fine)]


def angles(coarse_ref, fine_ref, first):
    at = pl.ds(pl.multiple_of(first // FINE, TILE // FINE), TILE // FINE)
    cos_a, sin_a = coarse_ref[0, at, :][:, None, :], coarse_ref[1, at, :][:, None, :]
    cos_b, sin_b = fine_ref[0][None], fine_ref[1][None]
    shape = (TILE, fine_ref.shape[2])
    return (cos_a * cos_b - sin_a * sin_b).reshape(shape), (sin_a * cos_b + cos_a * sin_b).reshape(shape)


def whole(shape):
    return pl.BlockSpec(shape, lambda *_: (0,) * len(shape))


def tiles(rows, columns):
    return pl.BlockSpec((rows, columns), lambda i, *_: (i, 0))


def hidden(b):
    return lax.broadcasted_iota(jnp.int32, (b, b), 0) <= lax.broadcasted_iota(jnp.int32, (b, b), 1)


def packed(full, layout, first, last=None):
    start, end = layout.span(first, last)
    return pl.BlockSpec((full.shape[0], end - start, full.shape[2]), lambda *_: (0, start // (end - start), 0))


def matrix(ref, first, rows):
    value = ref[:, first : first + rows, :] if len(ref.shape) == 3 else ref[:, :, first : first + rows, :]
    return value.reshape(-1, value.shape[-1])


def slots_of(tokens, layout):
    n = tokens // TILE
    return n + n * (n + 1) // 2, n * layout.at["w_gate"][2]


def forward(x, layout, coarse, fine, layers, side, ident):
    tokens, d = x.shape
    b, width = TILE, layout.width
    heads = width // HEAD
    e = HEAD**-0.5 * LOG2E
    steps = tokens // b
    _, r, parts = layout.at["w_gate"]
    ff = parts * width
    _, small = layout.span("wq", "wv")
    chips = side.devices // 2
    some = side.devices // parts
    r_down = layout.at["w_down"][1]
    look_slots, feed_slots = slots_of(tokens, layout)
    every_layer = [n * (look_slots + feed_slots) for n in range(layers)]
    base = [i + i * (i + 1) // 2 for i in range(steps)]
    sites = lambda *at: [n + one for n in every_layer for one in at]

    def prepare(*scratch):
        w_s, rest_s, sem = scratch[-3:]

        def load(u):
            unit = side.units[u]
            first, end = unit["span"]
            target = w_s if end <= small else rest_s
            to = first if end <= small else first - small
            return pltpu.make_async_copy(
                side.full[unit["layer"]].at[:, :, pl.ds(first, end - first), :], target.at[:, :, pl.ds(to, end - first), :], sem.at[u])

        side.load = load
        side.then = lambda u: load(u).start()

    def wait(i, when, early):
        for n in range(layers):

            @pl.when(i == n * 2 * steps + when)
            def _():
                for u, unit in enumerate(side.units):
                    if unit["layer"] == n and (unit["span"][1] <= small) == early:
                        side.load(u).wait()

    def body(poke, x_ref, coarse_ref, fine_ref, q_ref, k_ref, v_ref, o_ref, lse_ref, h1_ref, gate_ref, up_ref, hn_ref,
             h_s, o_s, k_s, v_s, top_s, mix_s, w_s, rest_s, sem):
        i = pl.program_id(0)
        layer, within = i // (2 * steps), lax.rem(i, 2 * steps)
        zero = layer * (look_slots + feed_slots)
        wait(i, 0, True)
        wait(i, steps, False)

        @pl.when(within < steps)
        def _():
            iq = within
            slot = zero + iq + iq * (iq + 1) // 2
            poke(slot, sites(*base))
            mine = pl.ds(pl.multiple_of(iq * b, b), b)

            @pl.when(layer == 0)
            def _():
                h_s[mine, :] = x_ref[...]

            wide = h_s[mine, :].astype(f32)
            a = (wide * scale_of(wide)).astype(bf16)
            cos, sin = angles(coarse_ref, fine_ref, iq * b)
            for n, (out, all_s) in enumerate(((q_ref, None), (k_ref, k_s), (v_ref, v_s))):
                t = dot(a, matrix(w_s, n * r, r)).astype(bf16)
                for m in range(heads):
                    one = t[:, m * HEAD : (m + 1) * HEAD]
                    one = one if n == 2 else turn(one, cos, sin)
                    out[m] = one
                    if n:
                        all_s[m, mine, :] = one
            top_s[...] = jnp.full(top_s.shape, NEG, f32)
            mix_s[...] = jnp.zeros(mix_s.shape, f32)
            ones = jnp.ones((8, b), bf16)

            def block(j, masked):
                here = pl.ds(pl.multiple_of(j * b, b), b)
                scores = [dot(k_s[n, here, :], q_ref[n], 1, 1) for n in range(heads)]
                weights, keeps = [], []
                for n, s in enumerate(scores):
                    if masked:
                        s = jnp.where(hidden(b), s, 2 * NEG)
                    old = top_s[n : n + 1, :]
                    top = jnp.maximum(old, s.max(axis=0, keepdims=True))
                    top_s[n : n + 1, :] = top
                    weights.append(jnp.exp2((s - top) * e).astype(bf16))
                    keeps.append(jnp.exp2((old - top) * e))
                for n in range(heads):
                    values = jnp.concatenate([v_s[n, here, :].T, ones], axis=0)
                    mix_s[n] = mix_s[n] * keeps[n] + dot(values, weights[n])

            def seen(j, _):
                poke(slot + 1 + j, sites(*(base[n] + 1 + j for n in range(steps) for j in range(n))))
                block(j, False)

            lax.fori_loop(0, iq, seen, None)
            poke(slot + 1 + iq, sites(*(base[n] + 1 + n for n in range(steps))))
            block(iq, True)
            for n in range(heads):
                total = mix_s[n, HEAD : HEAD + 1, :]
                one = (mix_s[n, :HEAD, :] * (1 / total)).T.astype(bf16)
                o_ref[:, n * HEAD : (n + 1) * HEAD] = one
                o_s[mine, n * HEAD : (n + 1) * HEAD] = one
                lse_ref[n : n + 1, :] = top_s[n : n + 1, :] * HEAD**-0.5 + jnp.log(total)

        def feed(last):
            t = within - steps
            slot = zero + look_slots + parts * t
            mine = pl.ds(pl.multiple_of(t * b, b), b)
            poke(slot, sites(*(look_slots + parts * n for n in range(steps))))
            at_d, at_g, at_u = (layout.at[name][0] - small for name in ("w_down", "w_gate", "w_up"))
            h1 = h_s[mine, :] + dot(o_s[mine, :], matrix(rest_s, 0, r)).astype(bf16)
            h1_ref[...] = h1
            wide = h1.astype(f32)
            c = (wide * scale_of(wide)).astype(bf16)
            total = None
            for n in range(parts):
                if n:
                    poke(slot + n, sites(*(look_slots + parts * m + n for m in range(steps))))
                at = slice(n * width, (n + 1) * width)
                gate = dot(c, matrix(rest_s, at_g + n * r, r))
                up = dot(c, matrix(rest_s, at_u + n * r, r))
                gate_ref[:, at] = gate
                up_ref[:, at] = up
                if not last:
                    p = (gate * jax.nn.sigmoid(gate) * up).astype(bf16)
                    down = rest_s[n * some // 2 : (n + 1) * some // 2, :, at_d : at_d + r_down, :].reshape(width, d)
                    one = dot(p, down)
                    total = one if total is None else total + one
            if not last:
                h = h1 + total.astype(bf16)
                h_s[mine, :] = h
                hn_ref[...] = h

        for last in range(2):

            @pl.when((within >= steps) & ((layer == layers - 1) == bool(last)))
            def _():
                feed(last)

    which = lambda i: i // (2 * steps)
    early = lambda i: jnp.minimum(lax.rem(i, 2 * steps), steps - 1)
    late = lambda i: jnp.maximum(lax.rem(i, 2 * steps) - steps, 0)
    per_head = pl.BlockSpec((None, heads, b, HEAD), lambda i: (which(i), 0, early(i), 0))
    rows = lambda columns, when: pl.BlockSpec((None, b, columns), lambda i: (which(i), when(i), 0))
    ahead = lambda i: jnp.minimum(which(i), layers - 2)
    return run(
        body, layers * 2 * steps, [x, coarse, fine],
        [pl.BlockSpec((b, d), lambda i: (jnp.minimum(i, steps - 1), 0)), whole(coarse.shape), whole(fine.shape)],
        [sds((layers, heads, tokens, HEAD), bf16)] * 3 + [sds((layers, tokens, width), bf16), sds((layers, heads, tokens), f32)]
        + [sds((layers, tokens, d), bf16)] + [sds((layers, tokens, ff), f32)] * 2 + [sds((layers - 1, tokens, d), bf16)],
        [per_head] * 3 + [rows(width, early), pl.BlockSpec((None, heads, b), lambda i: (which(i), 0, early(i)))]
        + [rows(d, late)] + [rows(ff, late)] * 2
        + [pl.BlockSpec((None, b, d), lambda i: (ahead(i), jnp.where(which(i) > ahead(i), steps - 1, late(i)), 0))],
        [pltpu.VMEM((tokens, d), bf16), pltpu.VMEM((tokens, width), bf16)] + [pltpu.VMEM((heads, tokens, HEAD), bf16)] * 2
        + [pltpu.VMEM((heads, b), f32), pltpu.VMEM((heads, HEAD + 8, b), f32)]
        + [pltpu.VMEM((chips, 2, small, width), bf16), pltpu.VMEM((chips, 2, layout.rows - small, width), bf16)]
        + [pltpu.SemaphoreType.DMA((len(side.units),))],
        side=side, ident=ident, name="forward", slots=every_layer[-1] + look_slots + feed_slots, prepare=prepare,
        flops=layers * (6 * tokens * d * width + 2 * heads * tokens * tokens * HEAD + 2 * tokens * d * (d + 3 * ff)))


def of(layer, spec):
    return pl.BlockSpec((None,) + tuple(spec.block_shape), lambda *i: (layer, *spec.index_map(*i)))


def feed_back(layer, h1, gate, up, dh2, full, layout, side, ident, early):
    _, tokens, d = h1.shape
    ff = gate.shape[2]
    part, tile = 256, TILE
    steps = ff // part

    def body(poke, h1_ref, gate_ref, up_ref, dh2_ref, g_ref, u_ref, d_ref, dh1_ref, dgu_ref, dd_ref, b_s, p_s, dgate_s, dup_s, db_s):
        f = pl.program_id(0)
        poke(f, range(steps))

        @pl.when(f == 0)
        def _():
            for t in range(0, tokens, tile):
                wide = h1_ref[t : t + tile, :].astype(f32)
                b_s[t : t + tile, :] = (wide * scale_of(wide)).astype(bf16)
                db_s[t : t + tile, :] = jnp.zeros((tile, d), f32)

        for t in range(0, tokens, tile):
            here = slice(t, t + tile)
            dp = dot(dh2_ref[here, :], d_ref[...].reshape(part, d), 1, 1).astype(bf16).astype(f32)
            gate, up = gate_ref[here, :], up_ref[here, :]
            s = jax.nn.sigmoid(gate)
            soft = gate * s
            p_s[here, :] = (soft * up).astype(bf16)
            dup = (dp * soft).astype(bf16)
            dgate = (dp * up * (s + soft * (1 - s))).astype(bf16)
            dup_s[here, :] = dup
            dgate_s[here, :] = dgate
            db_s[here, :] += dot(dgate, g_ref[...].reshape(d, part), 1, 1) + dot(dup, u_ref[...].reshape(d, part), 1, 1)
        dd_ref[...] = dot(p_s[...], dh2_ref[...], 0, 0).astype(bf16)
        at = pl.ds(pl.multiple_of(f * part, part), part)
        for n, some_s in enumerate((dgate_s, dup_s)):
            one = dot(b_s[...], some_s[...], 0, 0).astype(bf16)
            dgu_ref[n] = one
            if side:
                side.term(early)[n, :, :, :, at] = one.reshape(*side.sources[early][1:4], part)

        @pl.when(f == steps - 1)
        def _():
            for t in range(0, tokens, tile):
                here = slice(t, t + tile)
                wide = h1_ref[here, :].astype(f32)
                dn = db_s[here, :].astype(bf16).astype(f32)
                scale = scale_of(wide)
                back = scale * dn - wide * (scale * scale * scale * jnp.mean(dn * wide, -1, keepdims=True))
                dh1_ref[here, :] = dh2_ref[here, :] + back.astype(bf16)

    columns = lambda rows: pl.BlockSpec((rows, part), lambda f: (0, f))
    down = pl.BlockSpec((part, d), lambda f: (f, 0))
    devices, _, width = full.shape
    _, r, pieces = layout.at["w_gate"]

    def slab(name):
        first, per = layout.at[name][0] // r, width // part
        return pl.BlockSpec((devices, r, part), lambda f: (0, first + f // per, lax.rem(f, per)))

    at, r_down, _ = layout.at["w_down"]
    return run(
        body, steps, [h1, gate, up, dh2, full, full, full],
        [of(layer, whole((tokens, d))), of(layer, columns(tokens)), of(layer, columns(tokens)), whole((tokens, d)), slab("w_gate"), slab("w_up"),
         pl.BlockSpec((part // r_down, r_down, width), lambda f: (f, at // r_down, 0))],
        [sds((tokens, d), bf16), sds((2, d, ff), bf16), sds((ff, d), bf16)],
        [whole((tokens, d)), pl.BlockSpec((2, d, part), lambda f: (0, 0, f)), down],
        [pltpu.VMEM((tokens, d), bf16)] + [pltpu.VMEM((tokens, part), bf16)] * 3 + [pltpu.VMEM((tokens, d), f32)],
        side=side, ident=ident, flops=12 * tokens * d * ff, name="feed_back", slots=steps)


def look_back(layer, h, q, k, v, o, lse, dh1, full, layout, coarse, fine, first, side, ident, units=None):
    tokens, d = h.shape
    heads = q.shape[1]
    width = heads * HEAD
    b = TILE
    scale = HEAD**-0.5
    e = scale * LOG2E
    half = tokens // b
    blocks = half * (half + 1) // 2
    grads = [sds((4, d, width), bf16)] if units is None else []
    r = layout.at["wq"][1]

    def body(poke, h_ref, q_ref, k_ref, v_ref, o_ref, lse_ref, dh1_ref, w_ref, wo_ref, coarse_ref, fine_ref, *rest):
        if units is None:
            grad_ref, *rest = rest
        if not first:
            dh_ref, back_s, dh1_s, *rest = rest
        k_s, v_s, dq_a, dk_s, dv_s, dq_s, do_s, dwo_s, h_s, a_s, t_s, sem = rest
        i = pl.program_id(0)
        slot = i * (i + 1) // 2
        fetch = [pltpu.make_async_copy(h_ref, h_s, sem.at[0])]

        def keep(n, value):
            if units is None:
                grad_ref[n] = value
            else:
                u, at = units[n]
                side.term(u)[at] = value.reshape(side.sources[u][1:])

        @pl.when(i == 0)
        def _():
            for one in fetch:
                one.start()
            dk_s[...] = jnp.zeros(dk_s.shape, f32)
            dv_s[...] = jnp.zeros(dv_s.shape, f32)
            dwo_s[...] = jnp.zeros(dwo_s.shape, f32)

        @pl.when(i < half)
        def _():
            mine = pl.ds(pl.multiple_of(i * b, b), b)
            k_s[:, mine, :] = k_ref[...]
            v_s[:, mine, :] = v_ref[...]
            if not first:
                dh1_s[mine, :] = dh1_ref[...]
            do_s[...] = dot(dh1_ref[...], matrix(wo_ref, 0, r), 1, 1).astype(bf16)
            dwo_s[...] += dot(o_ref[...], dh1_ref[...], 0, 0)
            deltas = []
            for n in range(heads):
                cut = slice(n * HEAD, (n + 1) * HEAD)
                deltas.append((do_s[:, cut].astype(f32) * o_ref[:, cut].astype(f32)).T.sum(axis=0, keepdims=True))
            dq_s[...] = jnp.zeros(dq_s.shape, f32)

            def block(j, masked):
                here = pl.ds(pl.multiple_of(j * b, b), b)
                dos = [do_s[:, n * HEAD : (n + 1) * HEAD] for n in range(heads)]
                scores = [dot(k_s[n, here, :], q_ref[n], 1, 1) for n in range(heads)]
                dps = [dot(v_s[n, here, :], dos[n], 1, 1) for n in range(heads)]
                for n in range(heads):
                    p = jnp.exp2(scores[n] * e - lse_ref[n : n + 1, :] * LOG2E)
                    if masked:
                        p = jnp.where(hidden(b), p, 0.0)
                    ds = (p * (dps[n] - deltas[n])).astype(bf16)
                    dv_s[n, here, :] += dot(p.astype(bf16), dos[n])
                    dk_s[n, here, :] += dot(ds, q_ref[n])
                    dq_s[n] += dot(k_s[n, here, :].T, ds)

            def seen(j, _):
                poke(slot + j, [m * (m + 1) // 2 + j for m in range(half) for j in range(m)])
                block(j, False)

            lax.fori_loop(0, i, seen, None)
            poke(slot + i, [m * (m + 1) // 2 + m for m in range(half)])
            block(i, True)
            for n in range(heads):
                dq_a[n, mine, :] = (dq_s[n] * scale).T.astype(bf16)

        @pl.when(i == half - 1)
        def _():
            keep(0, dwo_s[...].astype(bf16))
            fetch[0].wait()
            for t in range(0, tokens, b):
                wide = h_s[t : t + b, :].astype(f32)
                a_s[t : t + b, :] = (wide * scale_of(wide)).astype(bf16)

        for n in range(3):

            @pl.when(i == half + n)
            def _():
                poke(blocks + n, [blocks + n])
                for t in range(0, tokens, b):
                    here = slice(t, t + b)
                    if n == 0:
                        some = [dv_s[m, here, :].astype(bf16) for m in range(heads)]
                    else:
                        cos, sin = angles(coarse_ref, fine_ref, t)
                        some = [(dk_s[m, here, :] * scale).astype(bf16) if n == 1 else dq_a[m, here, :] for m in range(heads)]
                        some = [turn(one, cos, -sin) for one in some]
                    for m in range(heads):
                        t_s[here, m * HEAD : (m + 1) * HEAD] = some[m]
                    if not first:
                        part = dot(t_s[here, :], matrix(w_ref, (2 - n) * r, r), 1, 1)
                        if n < 2:
                            back_s[here, :] = part if n == 0 else back_s[here, :] + part
                        else:
                            wide = h_s[here, :].astype(f32)
                            size = scale_of(wide)
                            dn = (back_s[here, :] + part).astype(bf16).astype(f32)
                            back = size * dn - wide * (size * size * size * jnp.mean(dn * wide, -1, keepdims=True))
                            dh_ref[here, :] = dh1_s[here, :] + back.astype(bf16)
                keep(1 + n, dot(a_s[...], t_s[...], 0, 0).astype(bf16))

    early = lambda i: jnp.minimum(i, half - 1)
    block = of(layer, pl.BlockSpec((heads, b, HEAD), lambda i: (0, early(i), 0)))
    rows = lambda columns: pl.BlockSpec((b, columns), lambda i: (early(i), 0))
    return run(
        body, half + 3, [h, q, k, v, o, lse, dh1, full, full, coarse, fine],
        [ANY, block, block, block, of(layer, rows(width)), of(layer, pl.BlockSpec((heads, b), lambda i: (0, early(i)))), rows(d),
         packed(full, layout, "wq", "wv"), packed(full, layout, "wo"),
         whole(coarse.shape), whole(fine.shape)],
        grads + ([] if first else [sds((tokens, d), bf16)]),
        [whole(g.shape) for g in grads] + ([] if first else [whole((tokens, d))]),
        ([] if first else [pltpu.VMEM((tokens, d), f32), pltpu.VMEM((tokens, d), bf16)])
        + [pltpu.VMEM((heads, tokens, HEAD), bf16)] * 3 + [pltpu.VMEM((heads, tokens, HEAD), f32)] * 2
        + [pltpu.VMEM((heads, HEAD, b), f32), pltpu.VMEM((b, width), bf16), pltpu.VMEM((width, d), f32)]
        + [pltpu.VMEM((tokens, d), bf16), pltpu.VMEM((tokens, d), bf16), pltpu.VMEM((tokens, width), bf16), pltpu.SemaphoreType.DMA((1,))],
        side=side, ident=ident, flops=5 * heads * tokens * tokens * HEAD + (10 if first else 16) * tokens * d * width, name="look_back",
        slots=blocks + 3)


def adamw(weights, m, v, gradients):
    arrays, at = [], {}
    for array in (piece[0] for one in gradients for layer in one for piece in layer):
        if id(array) not in at:
            at[id(array)] = len(arrays)
            arrays.append(array)
    count = len(weights)

    def kernel(*refs):
        w_refs, m_refs, v_refs = (refs[i * count : (i + 1) * count] for i in range(3))
        g_refs = refs[3 * count : 3 * count + len(arrays)]
        outs = refs[3 * count + len(arrays) :]
        for i in range(count):
            for number, pieces in enumerate(gradients[i]):
                for array, index, first in pieces:
                    here = slice(first, first + array.shape[2])
                    g = g_refs[at[id(array)]][index].astype(f32)
                    w = w_refs[i][number, :, here].astype(f32)
                    new_m = 0.9 * m_refs[i][number, :, here] + 0.1 * g
                    new_v = 0.95 * v_refs[i][number, :, here] + 0.05 * g * g
                    step = new_m * lax.rsqrt(new_v + 1e-8) + 0.1 * w
                    outs[i][number, :, here] = (w - 0.02 * step).astype(bf16)
                    outs[count + i][number, :, here] = new_m
                    outs[2 * count + i][number, :, here] = new_v

    return pl.pallas_call(
        kernel,
        in_specs=[VMEM] * (3 * count + len(arrays)),
        out_specs=[VMEM] * (3 * count),
        out_shape=[sds(w.shape, bf16) for w in weights] + [sds(w.shape, f32) for w in weights] * 2,
        compiler_params=pltpu.CompilerParams(vmem_limit_bytes=63 * MIB),
        name="adamw",
    )(*weights, *m, *v, *arrays)


def every(start, gap, first=None, count=6):
    return [start] + [start + (gap if first is None else first) + gap * s for s in range(count - 1)]


PLANS = {
    "forward": [
        (0, "wq", "wv", False, [-90, -80, -70, -60, -50, -40, -30]),
        (0, "wo", "w_down", "fine", [-79, -69, -59, -49, 0, 5, 9]),
        (0, "w_gate", None, "fine", [-68, -58, -48, -38, 2, 7, 11]),
        (0, "w_up", None, "fine", [-57, -47, -37, 0.1, 4, 9, 13]),
        (1, "wq", "wv", True, [7, 9.5, 12, 14.5, 17, 17.1, 22, 25]),
        (1, "wo", "w_down", True, [8, 13, 18, 23, 28, 28.1, 33, 36]),
        (1, "w_gate", None, True, [9.5, 14.5, 19.5, 24.5, 29, 29.1, 36, 39]),
        (1, "w_up", None, True, [11, 16, 21, 26, 31, 31.1, 39, 42]),
    ],
    "feed_back": [
        [every(0, 1, 1), [0, 1, 3, 5, 7, 8], every(3, 1, 1)],
        [every(3, 1, 1)],
    ],
    "look_back": [
        [every(0, 2.4, 1), every(1, 2.4, 1), every(11, 1.5, 1), every(12, 1.2, 1), every(13, 1, 1)],
        [every(0, 2.4, 1)],
    ],
}
EARLY = 3


def gather(groups, devices, weights, plan):
    layout = Layout(weights)
    units = [dict(layer=layer, span=layout.span(first, last), share=share, at=at) for layer, first, last, share, at in plan]
    return Gather(groups, devices, weights, units)


def solution(mesh):
    groups, devices = mesh.shape["rep"], mesh.shape["dp"]

    def step(x, dy, *arrays):
        weights, m, v = (arrays[i : i + 7] for i in (0, 7, 14))
        layers = weights[0].shape[0]
        layout = Layout(weights)
        h = x[0]
        tokens, d = h.shape
        coarse, fine = table(tokens)
        idents = iter(range(64))

        def terms(g):
            m_, rows, columns = g.shape if g.ndim == 3 else (1,) + g.shape
            return g.reshape(m_, devices // 2, 2, rows // devices, columns)

        def scatter(plan, *units):
            units = [(u[0], u[1] if len(u) > 1 else (0, u[0][4] if isinstance(u[0], tuple) else u[0].shape[4])) for u in units]
            return Scatter(groups, devices, [(*unit, at) for unit, at in zip(units, plan, strict=True)])

        def blocks(full):
            return full.reshape(devices, *full.shape[2:])

        side = gather(groups, devices, weights, PLANS["forward"])
        (q, k, vv, o, lse, h1, gate, up, ahead), full = forward(h, layout, coarse, fine, layers, side, next(idents))
        dh, small = dy[0], []
        mine = [[None] * 7 for _ in range(layers)]
        for number in reversed(range(layers)):
            w = blocks(full[number])
            ff = gate.shape[2]
            low = ff * EARLY // 8
            early = ((2, devices // 2, 2, d // devices, ff), (0, low))
            side = scatter(PLANS["feed_back"][number], *((terms(g),) for g in small), early)
            (dh1, dgu, dd), got = feed_back(number, h1, gate, up, dh, w, layout, side, next(idents), len(small))
            if small:
                for name, (one, at) in zip((3, 2, 1, 0, 6), [(0, 0), (0, 1), (0, 2), (0, 3), (1, 0)]):
                    mine[number + 1][name] = [(got[one], at, 0)]
            mine[number][4:6] = [(got[-1], 0, 0)], [(got[-1], 1, 0)]
            units, own = [(terms(dgu), (low, ff))], None
            if number == 0:
                units += [(terms(dd),)] + [((m_, devices // 2, 2, d // devices, d),) for m_ in (2, 1, 1)]
                own = [(2, 0), (2, 1), (3, 0), (4, 0)]
            side = scatter(PLANS["look_back"][number], *units)
            got_own, got = look_back(number, ahead[number - 1] if number else h, q, k, vv, o, lse, dh1, w, layout, coarse, fine, number == 0, side, next(idents), own)
            for i in range(2):
                mine[number][4 + i].append((got[0], i, low))
            if number:
                grads, dh = got_own
                small = [grads, dd]
            else:
                mine[number][6] = [(got[1], 0, 0)]
                for name, (one, at) in zip((3, 2, 1, 0), own):
                    mine[number][name] = [(got[one], at, 0)]
        return tuple(adamw(weights, m, v, [[mine[number][i] for number in range(layers)] for i in range(7)]))

    states, cut = P(("rep", "dp"), None, None), P(None, "dp", None)
    return jax.shard_map(
        step,
        mesh=mesh,
        in_specs=(states, states) + (cut,) * 21,
        out_specs=(P("rep", "dp", None),) * 21,
        check_vma=False,
    )
```

```python
import functools

import jax
import jax.numpy as jnp
import numpy as np
from jax import lax
from jax.experimental import pallas as pl
from jax.experimental.pallas import tpu as pltpu
from jax.sharding import PartitionSpec as P

HEAD = 256
THETA = 10000
NAMES = ("wq", "wk", "wv", "wo", "w_gate", "w_up", "w_down")
LOG2E = 1.4426950408889634
NEG = -1e30
VMEM_LIMIT = 127 * 2**19
MESH = pl.DeviceIdType.MESH
bf16, f32 = jnp.bfloat16, jnp.float32
ANY = pl.BlockSpec(memory_space=pl.ANY)
VMEM = pl.BlockSpec(memory_space=pltpu.VMEM)


def dot(a, b, ca=1, cb=0):
    return lax.dot_general(a, b, (((ca,), (cb,)), ((), ())), preferred_element_type=f32)


def dot_last(a, b):
    return dot(a, b, 1, 1)


def dot_first(a, b):
    return dot(a, b, 0, 0)


def loop(count, body):
    lax.fori_loop(0, count, lambda n, _: body(n), None)


def head(n):
    return slice(n * HEAD, (n + 1) * HEAD)


def row(n):
    return slice(n, n + 1)


def sds(shape, dtype):
    return jax.ShapeDtypeStruct(shape, dtype)


class Place:
    def __init__(self, groups, devices):
        me = lax.axis_index("dp")
        self.me, self.chips = me, devices // 2
        self.z, self.c = me // 2, lax.rem(me, 2)
        self.right = dict(dp=lax.rem(me + 2, devices))
        self.left = dict(dp=lax.rem(me + devices - 2, devices))
        self.partner = dict(dp=me + 1 - 2 * self.c)
        group, side = lax.axis_index("rep"), round(groups**0.5)
        x, y = group // side, lax.rem(group, side)
        self.beside = dict(rep=group + 1 - 2 * lax.rem(y, 2))
        self.above = dict(rep=group + side - 2 * side * lax.rem(x, 2))
        self.colour = lax.rem(x + y, 2)

    def chip(self, away):
        return lax.rem(self.z + (away + self.chips), self.chips)


def hops(devices, flip):
    chips = devices // 2
    far, near = chips // 2, chips - 1 - chips // 2
    return (near, far) if flip else (far, near)


def remote(source, target, send, recv, to):
    return pltpu.make_async_remote_copy(src_ref=source, dst_ref=target, send_sem=send, recv_sem=recv, device_id=to, device_id_type=MESH)


class Layout:
    def __init__(self, weights):
        by_name = dict(zip(NAMES, weights))
        self.width, self.at, self.rows = weights[0].shape[2], {}, 0
        for name in ("wq", "wk", "wv", "wo", "w_down", "w_gate", "w_up"):
            _, r, n = by_name[name].shape
            self.at[name] = (self.rows, r, n // self.width)
            self.rows += r * (n // self.width)

    def span(self, first, last):
        start, (end, r, pieces) = self.at[first][0], self.at[last]
        return start, end + r * pieces


ALL = (1, 0)


class Gather:
    def __init__(self, groups, devices, weights, units):
        self.groups, self.devices, self.units = groups, devices, units
        self.layout, self.layers = Layout(weights), weights[0].shape[0]
        self.most = max(hops(devices, 0))
        chips = devices // 2
        self.outs, self.out_specs = [sds((self.layers, chips, 2, self.layout.rows, self.layout.width), bf16)], [ANY]
        self.ins, self.in_specs = list(weights), [whole(w.shape) for w in weights]
        slots = 3 * chips + 3
        self.scratch = [
            pltpu.VMEM((self.layers, self.layout.rows, self.layout.width), bf16),
            pltpu.SemaphoreType.DMA((len(units), slots)),
            pltpu.SemaphoreType.DMA((len(units), slots)),
            pltpu.SemaphoreType.DMA((len(units),)),
        ]

    def bind(self, ins, outs, scratch):
        self.shards, (self.full,) = ins, outs
        self.pack, self.send, self.recv, self.local = scratch

    def meet(self):
        for name, ref in zip(NAMES, self.shards):
            at, r, pieces = self.layout.at[name]
            for n in range(pieces):
                self.pack[:, at + n * r : at + (n + 1) * r, :] = ref[:, :, n * self.layout.width : (n + 1) * self.layout.width]
        p = Place(self.groups, self.devices)
        greet(p.left, p.right, p.partner, p.beside, p.above)

    def rows(self, u, part):
        first, end = self.units[u]["span"]
        pieces, number = part
        n = (end - first) // pieces
        return pl.ds(first, n) if pieces == 1 else pl.ds(pl.multiple_of(first + number * n, 8), n)

    def half(self, u, p):
        return (2, p.colour) if self.units[u]["share"] else ALL

    def flows(self, u, p):
        right, left = hops(self.devices, u % 2)
        return (right, 0, 1, p.right), (left, self.devices // 4, -1, p.left)

    def hand(self, u, slot, part, to, p):
        view = self.full.at[self.units[u]["layer"], :, p.c, self.rows(u, part), :]
        return remote(view, view, self.send.at[u, slot], self.recv.at[u, slot], to)

    def hear(self, u, slot, part, to, p, core):
        view = self.full.at[self.units[u]["layer"], :, core, self.rows(u, part), :]
        return remote(view, view, self.send.at[u, slot], self.recv.at[u, slot], to)

    def pass_on(self, u, s, count, slot, way, to, p):
        rows = self.rows(u, self.half(u, p))
        target = self.full.at[self.units[u]["layer"], p.chip(-way * s), p.c, rows, :]
        source = self.pack.at[self.units[u]["layer"], rows, :] if s == 0 else target
        return remote(source, target, self.send.at[u, slot + s], self.recv.at[u, slot + s], to)

    def fine(self, u):
        return self.units[u]["share"] == "fine"

    def quarters(self, u, p, theirs=False):
        n = p.chips
        k = 1 - p.colour if theirs else p.colour
        for count, slot, way, _ in self.flows(u, p):
            for s in range(1, count + 1):
                copies = []
                for i, to in enumerate((p.beside, p.above)):
                    view = self.full.at[self.units[u]["layer"], p.chip(-way * s), p.c, self.rows(u, (4, 2 * k + i)), :]
                    at = n + 3 + i * n + slot + s - 1
                    copies.append(remote(view, view, self.send.at[u, at], self.recv.at[u, at], to))
                yield s, copies

    def keep(self, u, p):
        rows = self.rows(u, ALL if self.fine(u) else self.half(u, p))
        return pltpu.make_async_copy(self.pack.at[self.units[u]["layer"], rows, :], self.full.at[self.units[u]["layer"], p.z, p.c, rows, :], self.local.at[u])

    def ring(self, u, s):
        p = Place(self.groups, self.devices)
        if s == 0:
            self.keep(u, p).start()
        for count, slot, way, to in self.flows(u, p):
            if 0 < s <= count:
                view = self.full.at[self.units[u]["layer"], p.chip(-way * s), p.c, self.rows(u, self.half(u, p)), :]
                remote(view, view, self.send.at[u, slot + s - 1], self.recv.at[u, slot + s - 1], to).wait_recv()
            if s < count:
                self.pass_on(u, s, count, slot, way, to, p).start()
        if self.fine(u):
            for hop, copies in self.quarters(u, p):
                if hop == s:
                    for copy in copies:
                        copy.start()
        if s == self.most:
            self.keep(u, p).wait()
            for count, slot, way, to in self.flows(u, p):
                for t in range(count):
                    self.pass_on(u, t, count, slot, way, to, p).wait_send()

    def across(self, u, stage):
        p = Place(self.groups, self.devices)
        n, k = p.chips, p.colour
        share = self.units[u]["share"]
        if stage == 0 and share:
            self.hand(u, n, (4, 2 * k), p.beside, p).start()
            self.hand(u, n + 1, (4, 2 * k + 1), p.above, p).start()
        if stage == 1:
            if self.fine(u):
                for _, copies in self.quarters(u, p, theirs=True):
                    for copy in copies:
                        copy.wait_recv()
            elif share:
                self.hear(u, n, (4, 2 - 2 * k), p.beside, p, p.c).wait_recv()
                self.hear(u, n + 1, (4, 3 - 2 * k), p.above, p, p.c).wait_recv()
            self.hand(u, n + 2, ALL, p.partner, p).start()
        if stage == 2:
            self.hear(u, n + 2, ALL, p.partner, p, 1 - p.c).wait_recv()
            self.hand(u, n + 2, ALL, p.partner, p).wait_send()
            if self.fine(u):
                for _, copies in self.quarters(u, p):
                    for copy in copies:
                        copy.wait_send()
            elif share:
                self.hand(u, n, (4, 2 * k), p.beside, p).wait_send()
                self.hand(u, n + 1, (4, 2 * k + 1), p.above, p).wait_send()
            self.then(u)

    def steps(self):
        out = []
        for u, unit in enumerate(self.units):
            todo = [functools.partial(self.ring, u, s) for s in range(self.most + 1)]
            todo += [functools.partial(self.across, u, stage) for stage in range(0 if unit["share"] is True else 1, 3)]
            out += zip(unit["at"], todo, strict=True)
        return sorted(out, key=lambda one: one[0])


def greet(*others):
    barrier = pltpu.get_barrier_semaphore()
    for other in others:
        pl.semaphore_signal(barrier, inc=1, device_id=other, device_id_type=MESH)
    pl.semaphore_wait(barrier, len(others))


ROWS = 16


class Scatter:
    ins, in_specs = [], []

    def __init__(self, groups, devices, buffers, units):
        self.groups, self.devices, self.units = groups, devices, units
        self.most = max(hops(devices, 0))
        self.outs, self.out_specs = [], []
        for unit in units:
            shape = (unit["m"][1] - unit["m"][0], buffers[unit["buffer"]][3], unit["columns"][1] - unit["columns"][0])
            self.outs.append(sds(shape, bf16))
            self.out_specs.append(whole(shape))
        self.scratch = []
        for m, chips, two, r, n in buffers:
            self.scratch += [pltpu.VMEM((m, chips, two, r, n), bf16), pltpu.VMEM((m, chips, r, n), bf16), pltpu.VMEM((chips, m, r, n), bf16)]
        slots = devices // 2 + 1
        self.scratch += [pltpu.SemaphoreType.DMA((len(units), slots))] * 2 + [pltpu.SemaphoreType.REGULAR((len(units),))]

    def bind(self, ins, outs, scratch):
        self.result = outs
        *buffers, self.send, self.recv, self.free = scratch
        self.term, self.pair, self.come = buffers[0::3], buffers[1::3], buffers[2::3]

    def meet(self):
        p = Place(self.groups, self.devices)
        greet(p.left, p.right, p.partner)

    def parts(self, u):
        unit = self.units[u]
        at = unit["buffer"]
        m, columns = (pl.ds(first, end - first) for first, end in (unit["m"], unit["columns"]))
        return self.term[at], self.pair[at], self.come[at], m, columns

    def flows(self, u, p):
        right, left = hops(self.devices, u % 2)
        return (right, 0, 1, p.right), (left, self.devices // 4, -1, p.left)

    def swap(self, u, p):
        term, pair, _, m, columns = self.parts(u)
        slot = self.devices // 2
        return remote(term.at[m, :, 1 - p.c, :, columns], pair.at[m, :, :, columns], self.send.at[u, slot], self.recv.at[u, slot], p.partner)

    def copy(self, u, slot, chip, to):
        _, pair, come, m, columns = self.parts(u)
        return remote(pair.at[m, chip, :, columns], come.at[slot, m, :, columns], self.send.at[u, slot], self.recv.at[u, slot], to)

    def add_up(self, u, chip, slots, p, put):
        term, pair, come, _, columns = self.parts(u)
        first, end = self.units[u]["m"]
        pieces = term.shape[3] // ROWS

        def piece(number):
            i, rows = first + number // pieces, pl.ds(pl.multiple_of(lax.rem(number, pieces) * ROWS, ROWS), ROWS)
            total = term[i, chip, p.c, rows, columns].astype(f32) + pair[i, chip, rows, columns].astype(f32)
            for slot in slots:
                total += come[slot, i, rows, columns].astype(f32)
            put(i, rows, total.astype(bf16))

        loop((end - first) * pieces, piece)

    def first(self, u):
        p = Place(self.groups, self.devices)
        if self.units[u]["after"] is not None:
            pl.semaphore_wait(self.free.at[self.units[u]["after"]], 3)
        self.swap(u, p).start()

    def hop(self, u, s):
        p = Place(self.groups, self.devices)
        _, pair, _, _, columns = self.parts(u)
        if s == 1:
            self.swap(u, p).wait_recv()
        for count, slot, way, to in self.flows(u, p):
            if s > count:
                continue
            chip = p.chip(way * (count - s + 1))
            if s > 1:
                self.copy(u, slot + s - 2, chip, to).wait_recv()

            def put(i, rows, value):
                pair[i, chip, rows, columns] = value

            self.add_up(u, chip, [slot + s - 2] if s > 1 else [], p, put)
            self.copy(u, slot + s - 1, chip, to).start()

    def last(self, u):
        p = Place(self.groups, self.devices)
        self.swap(u, p).wait_send()
        slots = []
        for count, slot, _, to in self.flows(u, p):
            self.copy(u, slot + count - 1, p.z, to).wait_recv()
            slots.append(slot + count - 1)

        def put(i, rows, value):
            self.result[u][i - self.units[u]["m"][0], rows, :] = value

        self.add_up(u, p.z, slots, p, put)
        for count, slot, way, to in self.flows(u, p):
            for s in range(count):
                self.copy(u, slot + s, p.chip(way * (count - s)), to).wait_send()
        if any(unit["after"] == u for unit in self.units):
            for other in (p.left, p.right, p.partner):
                pl.semaphore_signal(self.free.at[u], inc=1, device_id=other, device_id_type=MESH)

    def steps(self):
        out = []
        for u, unit in enumerate(self.units):
            todo = [functools.partial(self.first, u)] + [functools.partial(self.hop, u, s) for s in range(1, self.most + 1)]
            out += zip(unit["at"], todo + [functools.partial(self.last, u)], strict=True)
        return sorted(out, key=lambda one: one[0])


def run(body, grid, ins, in_specs, outs, out_specs, scratch, side, ident, flops, name, times, prepare=None):
    counts = [len(some) for some in (ins, side.ins, outs, side.outs, scratch, side.scratch)]

    def kernel(*refs):
        parts, at = [], 0
        for n in counts:
            parts.append(list(refs[at : at + n]))
            at += n
        due, early, end = {}, [], []
        my_ins, side_ins, my_outs, side_outs, mine, its = parts
        side.bind(side_ins, side_outs, its)
        if prepare:
            prepare(*mine)
        for when, one in side.steps():
            slot = int(np.searchsorted(times, when))
            if when < 0:
                early.append(one)
            elif slot < len(times):
                due.setdefault(slot, []).append(one)
            else:
                end.append(one)

        step = pl.program_id(0)

        @pl.when(step == 0)
        def _():
            side.meet()
            for one in early:
                one()

        def poke(number, among):
            def choose(some):
                if len(some) == 1:

                    @pl.when(number == some[0])
                    def _():
                        for one in due[some[0]]:
                            one()
                elif some:
                    middle = len(some) // 2
                    lax.cond(number < some[middle], lambda: choose(some[:middle]), lambda: choose(some[middle:]))

            choose(sorted(at for at in among if at in due))

        body(poke, *my_ins, *my_outs, *mine)

        @pl.when(step == grid - 1)
        def _():
            for one in end:
                one()

    got = pl.pallas_call(
        kernel,
        grid=(grid,),
        in_specs=in_specs + side.in_specs,
        out_specs=out_specs + side.out_specs,
        out_shape=outs + side.outs,
        scratch_shapes=scratch + side.scratch,
        compiler_params=pltpu.CompilerParams(
            dimension_semantics=("arbitrary",), vmem_limit_bytes=VMEM_LIMIT, collective_id=ident, has_side_effects=True),
        cost_estimate=pl.CostEstimate(flops=flops, bytes_accessed=sum(a.size * a.dtype.itemsize for a in (*ins, *outs)), transcendentals=0),
        name=name,
    )(*ins, *side.ins)
    return got[: len(outs)], got[len(outs) :]


TILE = 512
FINE = 64


def scale_of(wide):
    return lax.rsqrt(jnp.mean(wide * wide, -1, keepdims=True) + 1e-6)


def turn(t, cos, sin):
    half = t.shape[-1] // 2
    a, b = t[:, :half].astype(f32), t[:, half:].astype(f32)
    return jnp.concatenate([a * cos - b * sin, b * cos + a * sin], -1).astype(bf16)


def table(tokens):
    half = HEAD // 2
    rate = np.float64(THETA) ** (-np.arange(half) / half)
    coarse, fine = (np.arange(n)[:, None] * step * rate for n, step in ((tokens // FINE, FINE), (FINE, 1)))
    return [jnp.asarray(np.stack([np.cos(a), np.sin(a)]).astype(np.float32)) for a in (coarse, fine)]


def angles(coarse_ref, fine_ref, first):
    at = pl.ds(pl.multiple_of(first // FINE, TILE // FINE), TILE // FINE)
    cos_a, sin_a = coarse_ref[0, at, :][:, None, :], coarse_ref[1, at, :][:, None, :]
    cos_b, sin_b = fine_ref[0][None], fine_ref[1][None]
    shape = (TILE, fine_ref.shape[2])
    return (cos_a * cos_b - sin_a * sin_b).reshape(shape), (sin_a * cos_b + cos_a * sin_b).reshape(shape)


def whole(shape):
    return pl.BlockSpec(shape, lambda *_: (0,) * len(shape))


def tiles(rows, columns):
    return pl.BlockSpec((rows, columns), lambda i, *_: (i, 0))


def hidden(b):
    return lax.broadcasted_iota(jnp.int32, (b, b), 0) <= lax.broadcasted_iota(jnp.int32, (b, b), 1)


def matrix(ref, first, rows):
    value = ref[:, first : first + rows, :] if len(ref.shape) == 3 else ref[:, :, first : first + rows, :]
    return value.reshape(-1, value.shape[-1])


def slots_of(tokens, layout):
    n = tokens // TILE
    return n + n * (n + 1) // 2, n * layout.at["w_gate"][2]


def forward(x, layout, coarse, fine, layers, side, ident):
    tokens, d = x.shape
    b, width = TILE, layout.width
    heads = width // HEAD
    e = HEAD**-0.5 * LOG2E
    steps = tokens // b
    _, r, parts = layout.at["w_gate"]
    ff = parts * width
    _, small = layout.span("wq", "wv")
    chips = side.devices // 2
    some = side.devices // parts
    r_down = layout.at["w_down"][1]
    look_slots, feed_slots = slots_of(tokens, layout)
    each = 2 * steps
    every_layer = [n * (look_slots + feed_slots) for n in range(layers)]
    base = [i + i * (i + 1) // 2 for i in range(steps)]
    sites = lambda *at: [n + one for n in every_layer for one in at]

    def prepare(*scratch):
        w_s, rest_s, sem = scratch[-3:]

        def load(u):
            unit = side.units[u]
            first, end = unit["span"]
            target = w_s if end <= small else rest_s
            to = first if end <= small else first - small
            return pltpu.make_async_copy(
                side.full.at[unit["layer"], :, :, pl.ds(first, end - first), :], target.at[:, :, pl.ds(to, end - first), :], sem.at[u])

        side.load = load
        side.then = lambda u: load(u).start()

    def wait(i, when, early):
        for n in range(layers):

            @pl.when(i == n * each + when)
            def _():
                for u, unit in enumerate(side.units):
                    if unit["layer"] == n and (unit["span"][1] <= small) == early:
                        side.load(u).wait()

    def body(poke, x_ref, coarse_ref, fine_ref, q_ref, k_ref, v_ref, o_ref, lse_ref, h1_ref, gate_ref, up_ref, hn_ref,
             h_s, o_s, k_s, v_s, top_s, mix_s, w_s, rest_s, sem):
        i = pl.program_id(0)
        layer, within = i // each, lax.rem(i, each)
        zero = layer * (look_slots + feed_slots)
        wait(i, 0, True)
        wait(i, steps, False)

        @pl.when(within < steps)
        def _():
            iq = within
            slot = zero + iq + iq * (iq + 1) // 2
            poke(slot, sites(*base))
            mine = pl.ds(pl.multiple_of(iq * b, b), b)

            @pl.when(layer == 0)
            def _():
                h_s[mine, :] = x_ref[:]

            wide = h_s[mine, :].astype(f32)
            a = (wide * scale_of(wide)).astype(bf16)
            cos, sin = angles(coarse_ref, fine_ref, iq * b)
            for n, (out, all_s) in enumerate(((q_ref, None), (k_ref, k_s), (v_ref, v_s))):
                t = dot(a, matrix(w_s, n * r, r)).astype(bf16)
                for m in range(heads):
                    one = t[:, head(m)]
                    one = one if n == 2 else turn(one, cos, sin)
                    out[m] = one
                    if n:
                        all_s[m, mine, :] = one
            top_s[:] = jnp.full(top_s.shape, NEG, f32)
            mix_s[:] = jnp.zeros(mix_s.shape, f32)
            ones = jnp.ones((8, b), bf16)

            def block(j, masked):
                here = pl.ds(pl.multiple_of(j * b, b), b)
                scores = [dot_last(k_s[n, here, :], q_ref[n]) for n in range(heads)]
                weights, keeps = [], []
                for n, s in enumerate(scores):
                    if masked:
                        s = jnp.where(hidden(b), s, 2 * NEG)
                    old = top_s[row(n), :]
                    top = jnp.maximum(old, s.max(axis=0, keepdims=True))
                    top_s[row(n), :] = top
                    weights.append(jnp.exp2((s - top) * e).astype(bf16))
                    keeps.append(jnp.exp2((old - top) * e))
                for n in range(heads):
                    values = jnp.concatenate([v_s[n, here, :].T, ones], axis=0)
                    mix_s[n] = mix_s[n] * keeps[n] + dot(values, weights[n])

            def seen(j):
                poke(slot + 1 + j, sites(*(base[n] + 1 + j for n in range(steps) for j in range(n))))
                block(j, False)

            loop(iq, seen)
            poke(slot + 1 + iq, sites(*(base[n] + 1 + n for n in range(steps))))
            block(iq, True)
            for n in range(heads):
                total = mix_s[n, HEAD : HEAD + 1, :]
                one = (mix_s[n, :HEAD, :] * (1 / total)).T.astype(bf16)
                o_ref[:, head(n)] = one
                o_s[mine, head(n)] = one
                lse_ref[row(n), :] = top_s[row(n), :] * HEAD**-0.5 + jnp.log(total)

        def feed(last):
            t = within - steps
            slot = zero + look_slots + parts * t
            mine = pl.ds(pl.multiple_of(t * b, b), b)
            poke(slot, sites(*(look_slots + parts * n for n in range(steps))))
            at_d, at_g, at_u = (layout.at[name][0] - small for name in ("w_down", "w_gate", "w_up"))
            h1 = h_s[mine, :] + dot(o_s[mine, :], matrix(rest_s, 0, r)).astype(bf16)
            h1_ref[:] = h1
            wide = h1.astype(f32)
            c = (wide * scale_of(wide)).astype(bf16)
            total = None
            for n in range(parts):
                if n:
                    poke(slot + n, sites(*(look_slots + parts * m + n for m in range(steps))))
                at = slice(n * width, (n + 1) * width)
                gate = dot(c, matrix(rest_s, at_g + n * r, r))
                up = dot(c, matrix(rest_s, at_u + n * r, r))
                gate_ref[:, at] = gate
                up_ref[:, at] = up
                if not last:
                    p = (gate * jax.nn.sigmoid(gate) * up).astype(bf16)
                    down = rest_s[n * some // 2 : (n + 1) * some // 2, :, at_d : at_d + r_down, :].reshape(width, d)
                    one = dot(p, down)
                    total = one if total is None else total + one
            if not last:
                h = h1 + total.astype(bf16)
                h_s[mine, :] = h
                hn_ref[:] = h

        for last in range(2):

            @pl.when((within >= steps) & ((layer == layers - 1) == bool(last)))
            def _():
                feed(last)

    which = lambda i: i // each
    early = lambda i: jnp.minimum(lax.rem(i, each), steps - 1)
    late = lambda i: jnp.maximum(lax.rem(i, each) - steps, 0)
    per_head = pl.BlockSpec((None, heads, b, HEAD), lambda i: (which(i), 0, early(i), 0))
    rows = lambda columns, when: pl.BlockSpec((None, b, columns), lambda i: (which(i), when(i), 0))
    ahead = lambda i: jnp.minimum(which(i), layers - 2)
    return run(
        body, layers * each, [x, coarse, fine],
        [pl.BlockSpec((b, d), lambda i: (jnp.minimum(i, steps - 1), 0)), whole(coarse.shape), whole(fine.shape)],
        [sds((layers, heads, tokens, HEAD), bf16)] * 3 + [sds((layers, tokens, width), bf16), sds((layers, heads, tokens), f32)]
        + [sds((layers, tokens, d), bf16)] + [sds((layers, tokens, ff), f32)] * 2 + [sds((layers - 1, tokens, d), bf16)],
        [per_head] * 3 + [rows(width, early), pl.BlockSpec((None, heads, b), lambda i: (which(i), 0, early(i)))]
        + [rows(d, late)] + [rows(ff, late)] * 2
        + [pl.BlockSpec((None, b, d), lambda i: (ahead(i), jnp.where(which(i) > ahead(i), steps - 1, late(i)), 0))],
        [pltpu.VMEM((tokens, d), bf16), pltpu.VMEM((tokens, width), bf16)] + [pltpu.VMEM((heads, tokens, HEAD), bf16)] * 2
        + [pltpu.VMEM((heads, b), f32), pltpu.VMEM((heads, HEAD + 8, b), f32)]
        + [pltpu.VMEM((chips, 2, small, width), bf16), pltpu.VMEM((chips, 2, layout.rows - small, width), bf16)]
        + [pltpu.SemaphoreType.DMA((len(side.units),))],
        side, ident, name="forward", times=range(every_layer[-1] + look_slots + feed_slots), prepare=prepare,
        flops=layers * (6 * tokens * d * width + 2 * heads * tokens * tokens * HEAD + 2 * tokens * d * (d + 3 * ff)))


def backward(x, dy, saved, full, layout, coarse, fine, side, ident):
    q, k, v, o, lse, h1, gate, up, ahead = saved
    layers, tokens, d = h1.shape
    ff, heads, width = gate.shape[2], q.shape[1], layout.width
    b, part = TILE, HEAD
    scale = HEAD**-0.5
    e = scale * LOG2E
    half, parts = tokens // b, ff // part
    blocks = half * (half + 1) // 2
    steps, slots = parts + half + 3, parts + blocks + 3
    r, r_down = layout.at["wq"][1], layout.at["w_down"][1]
    devices, chips = side.devices, side.devices // 2
    which = lambda i: layers - 1 - i // steps
    sites = lambda *at: [n * slots + one for n in range(layers) for one in at]

    def body(poke, x_ref, dy_ref, h1_ref, gate_ref, up_ref, ahead_ref, q_ref, k_ref, v_ref, o_ref, lse_ref, g_ref, u_ref, d_ref, w_ref, wo_ref,
             coarse_ref, fine_ref, dh_s, x_s, n_s, sum_s, kv_s, big_s, dq_a, dq_s, do_s, dwo_s, sem):
        i = pl.program_id(0)
        layer, within = which(i), lax.rem(i, steps)
        zero = (i // steps) * slots
        by_gu, by_d, by_small = side.term
        dk_s, dv_s = big_s.at[0], big_s.at[1]
        k_s, v_s = kv_s.at[0], kv_s.at[1]
        p_s, dgate_s, dup_s, t_s = k_s.at[0], k_s.at[1], v_s.at[0], k_s

        def tile(t):
            return pl.ds(pl.multiple_of(t * b, b), b)

        def chunk(layer, f):
            at, slot = pl.ds(pl.multiple_of(f * part, part), part), lax.rem(f, 2)
            return [pltpu.make_async_copy(ref.at[layer, :, at], big_s.at[slot, n], sem.at[slot, n]) for n, ref in enumerate((gate_ref, up_ref))]

        states = lambda: pltpu.make_async_copy(h1_ref.at[layer], x_s, sem.at[2, 0])
        first = lambda: pltpu.make_async_copy(dy_ref, dh_s, sem.at[2, 1])

        def inputs(start):
            for n in range(layers):

                @pl.when(layer == n)
                def _():
                    copy = pltpu.make_async_copy(ahead_ref.at[n - 1] if n else x_ref, x_s, sem.at[2, 0])
                    copy.start() if start else copy.wait()

        def norm(t):
            wide = x_s[tile(t), :].astype(f32)
            n_s[tile(t), :] = (wide * scale_of(wide)).astype(bf16)

        def norm_back(t):
            wide = x_s[tile(t), :].astype(f32)
            size = scale_of(wide)
            dn = sum_s[tile(t), :].astype(bf16).astype(f32)
            back = size * dn - wide * (size * size * size * jnp.mean(dn * wide, -1, keepdims=True))
            dh_s[tile(t), :] = dh_s[tile(t), :] + back.astype(bf16)

        @pl.when(within < parts)
        def _():
            f = within
            poke(zero + f, sites(*range(parts)))

            @pl.when(i == 0)
            def _():
                first().start()
                for copy in chunk(layer, f):
                    copy.start()

            @pl.when(f == 0)
            def _():
                states().start()
                sum_s[:] = jnp.zeros(sum_s.shape, f32)

            @pl.when(i == 0)
            def _():
                first().wait()

            for copy in chunk(layer, f):
                copy.wait()

            @pl.when(f < parts - 1)
            def _():
                for copy in chunk(layer, f + 1):
                    copy.start()

            @pl.when(f == 0)
            def _():
                states().wait()
                loop(half, norm)

            slot = lax.rem(f, 2)
            for t in range(half):
                here = slice(t * b, (t + 1) * b)
                dp = dot_last(dh_s[here, :], d_ref[:].reshape(part, d)).astype(bf16).astype(f32)
                gate, up = big_s[slot, 0, here, :], big_s[slot, 1, here, :]
                s = jax.nn.sigmoid(gate)
                soft = gate * s
                dup = (dp * soft).astype(bf16)
                dgate = (dp * up * (s + soft * (1 - s))).astype(bf16)
                p_s[here, :] = (soft * up).astype(bf16)
                dgate_s[here, :] = dgate
                dup_s[here, :] = dup
                sum_s[here, :] += dot_last(dgate, g_ref[:].reshape(d, part)) + dot_last(dup, u_ref[:].reshape(d, part))

            some = part // (2 * r_down)
            by_d[0, pl.ds(f * some, some)] = dot_first(p_s[:], dh_s[:]).astype(bf16).reshape(some, 2, r_down, d)
            at = pl.ds(pl.multiple_of(f * part, part), part)
            by_gu[0, :, :, :, at] = dot_first(n_s[:], dgate_s[:]).astype(bf16).reshape(chips, 2, r, part)
            by_gu[1, :, :, :, at] = dot_first(n_s[:], dup_s[:]).astype(bf16).reshape(chips, 2, r, part)

            @pl.when(f == parts - 1)
            def _():
                loop(half, norm_back)
                inputs(True)

        @pl.when((within >= parts) & (within < parts + half))
        def _():
            m = within - parts
            slot = zero + parts + m * (m + 1) // 2
            poke(slot, sites(*(parts + n * (n + 1) // 2 for n in range(half))))
            mine = tile(m)
            k_s[:, mine, :] = k_ref[:]
            v_s[:, mine, :] = v_ref[:]
            do_s[:] = dot_last(dh_s[mine, :], matrix(wo_ref, 0, r)).astype(bf16)
            one = dot_first(o_ref[:], dh_s[mine, :])
            dwo_s[:] = jnp.where(m == 0, one, dwo_s[:] + one)
            deltas = []
            for n in range(heads):
                cut = head(n)
                deltas.append((do_s[:, cut].astype(f32) * o_ref[:, cut].astype(f32)).T.sum(axis=0, keepdims=True))

            def block(j, diagonal):
                here = tile(j)
                dos = [do_s[:, head(n)] for n in range(heads)]
                scores = [dot_last(k_s[n, here, :], q_ref[n]) for n in range(heads)]
                dps = [dot_last(v_s[n, here, :], dos[n]) for n in range(heads)]
                for n in range(heads):
                    p = jnp.exp2(scores[n] * e - lse_ref[row(n), :] * LOG2E)
                    if diagonal:
                        p = jnp.where(hidden(b), p, 0.0)
                    ds = (p * (dps[n] - deltas[n])).astype(bf16)
                    for total, one in ((dv_s.at[n, here, :], dot(p.astype(bf16), dos[n])), (dk_s.at[n, here, :], dot(ds, q_ref[n])),
                                       (dq_s.at[n], dot(k_s[n, here, :].T, ds))):
                        total[:] = one if diagonal else total[:] + one

            block(m, True)

            def seen(j):
                poke(slot + 1 + j, sites(*(parts + n * (n + 1) // 2 + 1 + j for n in range(half) for j in range(n))))
                block(j, False)

            loop(m, seen)
            for n in range(heads):
                dq_a[n, mine, :] = (dq_s[n] * scale).T.astype(bf16)

        @pl.when(within == parts + half - 1)
        def _():
            by_small[0] = dwo_s[:].astype(bf16).reshape(chips, 2, r, d)
            inputs(False)
            loop(half, norm)

        @pl.when(within >= parts + half)
        def _():
            n = within - parts - half
            poke(zero + parts + blocks + n, sites(*range(parts + blocks, slots)))

            def made(number, source):
                @pl.when(n == number)
                def _():
                    def some(t):
                        cos, sin = (None, None) if number == 0 else angles(coarse_ref, fine_ref, t * b)
                        for m in range(heads):
                            one = source(m, tile(t))
                            t_s[m, tile(t), :] = one if number == 0 else turn(one, cos, -sin)

                    loop(half, some)

            made(0, lambda m, at: dv_s[m, at, :].astype(bf16))
            made(1, lambda m, at: (dk_s[m, at, :] * scale).astype(bf16))
            made(2, lambda m, at: dq_a[m, at, :])

            @pl.when((n == 2) & (layer > 0))
            def _():
                for copy in chunk(layer - 1, 0):
                    copy.start()

            for m in range(heads):
                cut = head(m)
                by_small[1 + n, :, :, :, cut] = dot_first(n_s[:], t_s[m]).astype(bf16).reshape(chips, 2, r, HEAD)

            @pl.when(layer > 0)
            def _():
                rows = pl.ds(pl.multiple_of((2 - n) * r, r), r)

                def back(t):
                    w = w_ref[:, rows, :].reshape(d, width)
                    one = sum(dot_last(t_s[m, tile(t), :], w[:, head(m)]) for m in range(heads))
                    sum_s[tile(t), :] = jnp.where(n == 0, one, sum_s[tile(t), :] + one)

                loop(half, back)

                @pl.when(n == 2)
                def _():
                    loop(half, norm_back)

    def spec(shape, index):
        return pl.BlockSpec((None,) + shape, lambda i: (which(i), *index(lax.rem(i, steps))))

    now = lambda w: jnp.minimum(w, parts - 1)
    query = lambda w: jnp.clip(w - parts, 0, half - 1)
    block = spec((heads, b, HEAD), lambda w: (0, query(w), 0))
    per = width // part

    def slab(name):
        first = layout.at[name][0] // r
        return spec((devices, r, part), lambda w: (0, first + now(w) // per, lax.rem(now(w), per)))

    def matrices(first, last):
        start, end = layout.span(first, last)
        return spec((devices, end - start, width), lambda w: (0, start // (end - start), 0))

    at_d = layout.at["w_down"][0]
    return run(
        body, layers * steps, [x, dy, h1, gate, up, ahead, q, k, v, o, lse, full, full, full, full, full, coarse, fine],
        [ANY] * 6 + [block] * 3 + [spec((b, width), lambda w: (query(w), 0)), spec((heads, b), lambda w: (0, query(w)))]
        + [slab("w_gate"), slab("w_up"), spec((part // r_down, r_down, width), lambda w: (now(w), at_d // r_down, 0))]
        + [matrices("wq", "wv"), matrices("wo", "wo"), whole(coarse.shape), whole(fine.shape)],
        [], [],
        [pltpu.VMEM((tokens, d), bf16)] * 3 + [pltpu.VMEM((tokens, d), f32), pltpu.VMEM((2, heads, tokens, HEAD), bf16)]
        + [pltpu.VMEM((2, 2, tokens, part), f32), pltpu.VMEM((heads, tokens, HEAD), bf16), pltpu.VMEM((heads, HEAD, b), f32)]
        + [pltpu.VMEM((b, width), bf16), pltpu.VMEM((width, d), f32), pltpu.SemaphoreType.DMA((3, 2))],
        side, ident, times=range(layers * slots), name="backward",
        flops=layers * (12 * tokens * d * ff + 5 * heads * tokens * tokens * HEAD + 16 * tokens * d * width))[1]


def adamw(weights, m, v, gradients):
    arrays, at = [], {}
    for array in (piece[0] for one in gradients for layer in one for piece in layer):
        if id(array) not in at:
            at[id(array)] = len(arrays)
            arrays.append(array)
    count = len(weights)

    def kernel(*refs):
        left = iter(refs)
        w_refs, m_refs, v_refs, g_refs, new_w, new_m, new_v = (
            [next(left) for _ in some] for some in (weights, m, v, arrays, weights, weights, weights))
        for i in range(count):
            for number, pieces in enumerate(gradients[i]):
                for array, index, first in pieces:
                    here = slice(first, first + array.shape[2])
                    g = g_refs[at[id(array)]][index].astype(f32)
                    w = w_refs[i][number, :, here].astype(f32)
                    moment = 0.9 * m_refs[i][number, :, here] + 0.1 * g
                    square = 0.95 * v_refs[i][number, :, here] + 0.05 * g * g
                    step = moment * lax.rsqrt(square + 1e-8) + 0.1 * w
                    new_w[i][number, :, here] = (w - 0.02 * step).astype(bf16)
                    new_m[i][number, :, here] = moment
                    new_v[i][number, :, here] = square

    return pl.pallas_call(
        kernel,
        in_specs=[VMEM] * (3 * count + len(arrays)),
        out_specs=[VMEM] * (3 * count),
        out_shape=[sds(w.shape, bf16) for w in weights] + [sds(w.shape, f32) for w in weights] * 2,
        compiler_params=pltpu.CompilerParams(vmem_limit_bytes=VMEM_LIMIT),
        name="adamw",
    )(*weights, *m, *v, *arrays)


def every(start, gap, count):
    return [start + gap * n for n in range(count)]


def forward_plan():
    ring, fetched = every(-90, 10, 7), [4, 6, 9, 11, 14, 14, 19, 24]
    plan = [(0, "wq", "wv", False, ring), (1, "wq", "wv", True, fetched)]
    for n, names in enumerate((("wo", "w_down"), ("w_gate", "w_gate"), ("w_up", "w_up"))):
        plan.append((0, *names, "fine", every(11 * n - 79, 10, 4) + [1, 6, 11]))
        plan.append((1, *names, True, [4, 9, 14, 19, 24, 24, 37, 41]))
    return plan


def backward_plan(parts, blocks, rows, columns):
    low, high, down, small = (0, columns // 2), (columns // 2, columns), (0, rows), (0, rows)
    two, one, half, each = (0, 2), (0, 1), parts // 2, parts + blocks + 3
    after = [parts + n for n in (0, 2, 5, 8)]
    plan = [(0, "low", 0, two, low, [*range(half, parts + 1), after[1]])]
    plan += [(0, name, at, m_, which, after + [each - 2, each]) for name, at, m_, which in (("high", 0, two, high), ("down", 1, one, down))]
    plan += [(0, "small", 2, (0, 4), small, [each + n for n in (0, 2, 4, 6, parts, parts + 2)])]
    plan += [(1, "low", 0, two, low, [each + n for n in (*range(half, parts + 1), after[1])])]
    now = [each + n for n in after]
    end = 2 * each
    plan += [(1, name, at, m_, which, now + [end - 2, end + 0.7]) for name, at, m_, which in (("high", 0, two, high), ("down", 1, one, down))]
    for name, first, last, start in (("small", 0, 2, -2), ("k", 2, 3, -1), ("q", 3, 4, 0)):
        due = [end + start, end + start + 1 if start else end + 0.5]
        plan.append((1, name, 2, (first, last), small, due + every(end + 1 + first / 10, 1, 4)))
    return plan


def gather(groups, devices, weights, plan):
    layout = Layout(weights)
    units = [dict(layer=layer, span=layout.span(first, last), share=share, at=at) for layer, first, last, share, at in plan]
    return Gather(groups, devices, weights, units)


def solution(mesh):
    groups, devices = mesh.shape["rep"], mesh.shape["dp"]

    def step(x, dy, *arrays):
        weights, m, v = (arrays[i : i + 7] for i in (0, 7, 14))
        layers = weights[0].shape[0]
        layout = Layout(weights)
        h = x[0]
        tokens, d = h.shape
        coarse, fine = table(tokens)
        idents = iter(range(64))

        side = gather(groups, devices, weights, forward_plan())
        saved, (full,) = forward(h, layout, coarse, fine, layers, side, next(idents))
        ff, half = saved[6].shape[2], tokens // TILE
        parts = ff // HEAD
        buffers = [(m_, devices // 2, 2, w.shape[1], w.shape[2]) for m_, w in zip((2, 1, 4), (weights[i] for i in map(NAMES.index, ("w_up", "w_down", "wq"))))]
        units, where = [], {}
        for n, name, buffer, m_, columns, at in backward_plan(parts, half * (half + 1) // 2, d, ff):
            where[layers - 1 - n, name] = len(units)
            units.append(dict(buffer=buffer, m=m_, columns=columns, at=at, after=where.get((layers - n, name))))
        got = backward(h, dy[0], saved, full.reshape(layers, devices, *full.shape[3:]), layout, coarse, fine,
                       Scatter(groups, devices, buffers, units), next(idents))

        def pieces(number, name):
            one = lambda unit, index, first=0: (got[where[number, unit]], index, first)
            if name in ("w_gate", "w_up"):
                return [one(unit, int(name == "w_up"), first) for unit, first in (("low", 0), ("high", ff // 2))]
            if name == "w_down":
                return [one("down", 0)]
            place = ("wo", "wv", "wk", "wq").index(name)
            own = name[1:] if (number, name[1:]) in where else "small"
            return [one(own, 0 if own != "small" else place)]

        return tuple(adamw(weights, m, v, [[pieces(number, name) for number in range(layers)] for name in NAMES]))

    states, cut = P(("rep", "dp")), P(None, "dp")
    return jax.shard_map(
        step,
        mesh=mesh,
        in_specs=(states, states) + (cut,) * 21,
        out_specs=(P("rep", "dp"),) * 21,
        check_vma=False,
    )
```

```python
import functools

import jax
import jax.numpy as jnp
import numpy as np
from jax import lax
from jax.experimental import pallas as pl
from jax.experimental.pallas import tpu as pltpu
from jax.sharding import PartitionSpec as P

HEAD = 256
THETA = 10000
NAMES = ("wq", "wk", "wv", "wo", "w_gate", "w_up", "w_down")
LOG2E = 1.4426950408889634
NEG = -1e30
VMEM_LIMIT = 127 * 2**19
MESH = pl.DeviceIdType.MESH
bf16, f32 = jnp.bfloat16, jnp.float32
ANY = pl.BlockSpec(memory_space=pl.ANY)


def dot(a, b, ca=1, cb=0):
    return lax.dot_general(a, b, (((ca,), (cb,)), ((), ())), preferred_element_type=f32)


def dot_last(a, b):
    return dot(a, b, 1, 1)


def dot_first(a, b):
    return dot(a, b, 0, 0)


def loop(count, body):
    lax.fori_loop(0, count, lambda n, _: body(n), None)


def head(n):
    return slice(n * HEAD, (n + 1) * HEAD)


def row(n):
    return slice(n, n + 1)


def sds(shape, dtype):
    return jax.ShapeDtypeStruct(shape, dtype)


class Place:
    def __init__(self, groups, devices):
        me = lax.axis_index("dp")
        self.me, self.chips = me, devices // 2
        self.z, self.c = me // 2, lax.rem(me, 2)
        self.right = dict(dp=lax.rem(me + 2, devices))
        self.left = dict(dp=lax.rem(me + devices - 2, devices))
        self.partner = dict(dp=me + 1 - 2 * self.c)
        group, side = lax.axis_index("rep"), round(groups**0.5)
        x, y = group // side, lax.rem(group, side)
        self.beside = dict(rep=group + 1 - 2 * lax.rem(y, 2))
        self.above = dict(rep=group + side - 2 * side * lax.rem(x, 2))
        self.colour = lax.rem(x + y, 2)

    def chip(self, away):
        return lax.rem(self.z + (away + self.chips), self.chips)


def hops(devices, flip):
    chips = devices // 2
    far, near = chips // 2, chips - 1 - chips // 2
    return (near, far) if flip else (far, near)


def remote(source, target, send, recv, to):
    return pltpu.make_async_remote_copy(src_ref=source, dst_ref=target, send_sem=send, recv_sem=recv, device_id=to, device_id_type=MESH)


class Layout:
    def __init__(self, weights):
        by_name = dict(zip(NAMES, weights))
        self.width, self.at, self.rows = weights[0].shape[2], {}, 0
        for name in ("wq", "wk", "wv", "wo", "w_down", "w_gate", "w_up"):
            _, r, n = by_name[name].shape
            self.at[name] = (self.rows, r, n // self.width)
            self.rows += r * (n // self.width)

    def span(self, first, last):
        start, (end, r, pieces) = self.at[first][0], self.at[last]
        return start, end + r * pieces


ALL = (1, 0)


class Gather:
    def __init__(self, groups, devices, weights, units):
        self.groups, self.devices, self.units = groups, devices, units
        self.layout, self.layers = Layout(weights), weights[0].shape[0]
        self.most = max(hops(devices, 0))
        chips = devices // 2
        self.outs, self.out_specs = [sds((self.layers, chips, 2, self.layout.rows, self.layout.width), bf16)], [ANY]
        self.ins, self.in_specs = list(weights), [whole(w.shape) for w in weights]
        slots = 3 * chips + 3
        self.scratch = [
            pltpu.VMEM((self.layers, self.layout.rows, self.layout.width), bf16),
            pltpu.SemaphoreType.DMA((len(units), slots)),
            pltpu.SemaphoreType.DMA((len(units), slots)),
            pltpu.SemaphoreType.DMA((len(units),)),
        ]

    def bind(self, ins, outs, scratch):
        self.shards, (self.full,) = ins, outs
        self.pack, self.send, self.recv, self.local = scratch

    def meet(self):
        for name, ref in zip(NAMES, self.shards):
            at, r, pieces = self.layout.at[name]
            for n in range(pieces):
                self.pack[:, at + n * r : at + (n + 1) * r, :] = ref[:, :, n * self.layout.width : (n + 1) * self.layout.width]
        p = Place(self.groups, self.devices)
        greet(p.left, p.right, p.partner, p.beside, p.above)

    def rows(self, u, part):
        first, end = self.units[u]["span"]
        pieces, number = part
        n = (end - first) // pieces
        return pl.ds(first, n) if pieces == 1 else pl.ds(pl.multiple_of(first + number * n, 8), n)

    def half(self, u, p):
        return (2, p.colour) if self.units[u]["share"] else ALL

    def flows(self, u, p):
        right, left = hops(self.devices, u % 2)
        return (right, 0, 1, p.right), (left, self.devices // 4, -1, p.left)

    def hand(self, u, slot, part, to, p):
        view = self.full.at[self.units[u]["layer"], :, p.c, self.rows(u, part), :]
        return remote(view, view, self.send.at[u, slot], self.recv.at[u, slot], to)

    def hear(self, u, slot, part, to, p, core):
        view = self.full.at[self.units[u]["layer"], :, core, self.rows(u, part), :]
        return remote(view, view, self.send.at[u, slot], self.recv.at[u, slot], to)

    def pass_on(self, u, s, count, slot, way, to, p):
        rows = self.rows(u, self.half(u, p))
        target = self.full.at[self.units[u]["layer"], p.chip(-way * s), p.c, rows, :]
        source = self.pack.at[self.units[u]["layer"], rows, :] if s == 0 else target
        return remote(source, target, self.send.at[u, slot + s], self.recv.at[u, slot + s], to)

    def fine(self, u):
        return self.units[u]["share"] == "fine"

    def quarters(self, u, p, theirs=False):
        n = p.chips
        k = 1 - p.colour if theirs else p.colour
        for count, slot, way, _ in self.flows(u, p):
            for s in range(1, count + 1):
                copies = []
                for i, to in enumerate((p.beside, p.above)):
                    view = self.full.at[self.units[u]["layer"], p.chip(-way * s), p.c, self.rows(u, (4, 2 * k + i)), :]
                    at = n + 3 + i * n + slot + s - 1
                    copies.append(remote(view, view, self.send.at[u, at], self.recv.at[u, at], to))
                yield s, copies

    def keep(self, u, p):
        rows = self.rows(u, ALL if self.fine(u) else self.half(u, p))
        return pltpu.make_async_copy(self.pack.at[self.units[u]["layer"], rows, :], self.full.at[self.units[u]["layer"], p.z, p.c, rows, :], self.local.at[u])

    def ring(self, u, s):
        p = Place(self.groups, self.devices)
        if s == 0:
            self.keep(u, p).start()
        for count, slot, way, to in self.flows(u, p):
            if 0 < s <= count:
                view = self.full.at[self.units[u]["layer"], p.chip(-way * s), p.c, self.rows(u, self.half(u, p)), :]
                remote(view, view, self.send.at[u, slot + s - 1], self.recv.at[u, slot + s - 1], to).wait_recv()
            if s < count:
                self.pass_on(u, s, count, slot, way, to, p).start()
        if self.fine(u):
            for hop, copies in self.quarters(u, p):
                if hop == s:
                    for copy in copies:
                        copy.start()
        if s == self.most:
            self.keep(u, p).wait()
            for count, slot, way, to in self.flows(u, p):
                for t in range(count):
                    self.pass_on(u, t, count, slot, way, to, p).wait_send()

    def across(self, u, stage):
        p = Place(self.groups, self.devices)
        n, k = p.chips, p.colour
        share = self.units[u]["share"]
        if stage == 0 and share:
            self.hand(u, n, (4, 2 * k), p.beside, p).start()
            self.hand(u, n + 1, (4, 2 * k + 1), p.above, p).start()
        if stage == 1:
            if self.fine(u):
                for _, copies in self.quarters(u, p, theirs=True):
                    for copy in copies:
                        copy.wait_recv()
            elif share:
                self.hear(u, n, (4, 2 - 2 * k), p.beside, p, p.c).wait_recv()
                self.hear(u, n + 1, (4, 3 - 2 * k), p.above, p, p.c).wait_recv()
            self.hand(u, n + 2, ALL, p.partner, p).start()
        if stage == 2:
            self.hear(u, n + 2, ALL, p.partner, p, 1 - p.c).wait_recv()
            self.hand(u, n + 2, ALL, p.partner, p).wait_send()
            if self.fine(u):
                for _, copies in self.quarters(u, p):
                    for copy in copies:
                        copy.wait_send()
            elif share:
                self.hand(u, n, (4, 2 * k), p.beside, p).wait_send()
                self.hand(u, n + 1, (4, 2 * k + 1), p.above, p).wait_send()
            self.then(u)

    def steps(self):
        out = []
        for u, unit in enumerate(self.units):
            todo = [functools.partial(self.ring, u, s) for s in range(self.most + 1)]
            todo += [functools.partial(self.across, u, stage) for stage in range(0 if unit["share"] is True else 1, 3)]
            out += zip(unit["at"], todo, strict=True)
        return sorted(out, key=lambda one: one[0])


def greet(*others):
    barrier = pltpu.get_barrier_semaphore()
    for other in others:
        pl.semaphore_signal(barrier, inc=1, device_id=other, device_id_type=MESH)
    pl.semaphore_wait(barrier, len(others))


ROWS = 32


class Scatter:
    ins, in_specs = [], []

    def __init__(self, groups, devices, buffers, units):
        self.groups, self.devices, self.units = groups, devices, units
        self.most = max(hops(devices, 0))
        self.outs, self.out_specs = [], []
        for unit in units:
            shape = (unit["m"][1] - unit["m"][0], buffers[unit["buffer"]][3], unit["columns"][1] - unit["columns"][0])
            self.outs.append(sds(shape, bf16))
            self.out_specs.append(whole(shape))
        self.scratch = []
        for m, chips, two, r, n in buffers:
            self.scratch += [pltpu.VMEM((m, chips, two, r, n), bf16), pltpu.VMEM((m, chips, r, n), bf16), pltpu.VMEM((chips, m, r, n), bf16)]
        slots = devices // 2 + 1
        self.scratch += [pltpu.SemaphoreType.DMA((len(units), slots))] * 2 + [pltpu.SemaphoreType.REGULAR((len(units),))]

    def bind(self, ins, outs, scratch):
        self.result = outs
        *buffers, self.send, self.recv, self.free = scratch
        self.term, self.pair, self.come = buffers[0::3], buffers[1::3], buffers[2::3]

    def meet(self):
        p = Place(self.groups, self.devices)
        greet(p.left, p.right, p.partner)

    def parts(self, u):
        unit = self.units[u]
        at = unit["buffer"]
        m, columns = (pl.ds(first, end - first) for first, end in (unit["m"], unit["columns"]))
        return self.term[at], self.pair[at], self.come[at], m, columns

    def flows(self, u, p):
        right, left = hops(self.devices, u % 2)
        return (right, 0, 1, p.right), (left, self.devices // 4, -1, p.left)

    def swap(self, u, p):
        term, pair, _, m, columns = self.parts(u)
        slot = self.devices // 2
        return remote(term.at[m, :, 1 - p.c, :, columns], pair.at[m, :, :, columns], self.send.at[u, slot], self.recv.at[u, slot], p.partner)

    def copy(self, u, slot, chip, to):
        _, pair, come, m, columns = self.parts(u)
        return remote(pair.at[m, chip, :, columns], come.at[slot, m, :, columns], self.send.at[u, slot], self.recv.at[u, slot], to)

    def add_up(self, u, chip, slots, p, put):
        term, pair, come, _, columns = self.parts(u)
        first, end = self.units[u]["m"]
        pieces = term.shape[3] // ROWS

        def piece(number):
            i, rows = first + number // pieces, pl.ds(pl.multiple_of(lax.rem(number, pieces) * ROWS, ROWS), ROWS)
            total = term[i, chip, p.c, rows, columns].astype(f32) + pair[i, chip, rows, columns].astype(f32)
            for slot in slots:
                total += come[slot, i, rows, columns].astype(f32)
            put(i, rows, total.astype(bf16))

        loop((end - first) * pieces, piece)

    def first(self, u):
        p = Place(self.groups, self.devices)
        if self.units[u]["after"] is not None:
            pl.semaphore_wait(self.free.at[self.units[u]["after"]], 3)
        self.swap(u, p).start()

    def hop(self, u, s):
        p = Place(self.groups, self.devices)
        _, pair, _, _, columns = self.parts(u)
        if s == 1:
            self.swap(u, p).wait_recv()
        for count, slot, way, to in self.flows(u, p):
            if s > count:
                continue
            chip = p.chip(way * (count - s + 1))
            if s > 1:
                self.copy(u, slot + s - 2, chip, to).wait_recv()

            def put(i, rows, value):
                pair[i, chip, rows, columns] = value

            self.add_up(u, chip, [slot + s - 2] if s > 1 else [], p, put)
            self.copy(u, slot + s - 1, chip, to).start()

    def last(self, u):
        p = Place(self.groups, self.devices)
        self.swap(u, p).wait_send()
        slots = []
        for count, slot, _, to in self.flows(u, p):
            self.copy(u, slot + count - 1, p.z, to).wait_recv()
            slots.append(slot + count - 1)

        def put(i, rows, value):
            self.result[u][i - self.units[u]["m"][0], rows, :] = value

        self.add_up(u, p.z, slots, p, put)
        for count, slot, way, to in self.flows(u, p):
            for s in range(count):
                self.copy(u, slot + s, p.chip(way * (count - s)), to).wait_send()
        if any(unit["after"] == u for unit in self.units):
            for other in (p.left, p.right, p.partner):
                pl.semaphore_signal(self.free.at[u], inc=1, device_id=other, device_id_type=MESH)

    def steps(self):
        out = []
        for u, unit in enumerate(self.units):
            todo = [functools.partial(self.first, u)] + [functools.partial(self.hop, u, s) for s in range(1, self.most + 1)]
            out += zip(unit["at"], todo + [functools.partial(self.last, u)], strict=True)
        return sorted(out, key=lambda one: one[0])


def run(body, grid, ins, in_specs, outs, out_specs, scratch, side, ident, flops, name, times, prepare=None):
    counts = [len(some) for some in (ins, side.ins, outs, side.outs, scratch, side.scratch)]

    def kernel(*refs):
        parts, at = [], 0
        for n in counts:
            parts.append(list(refs[at : at + n]))
            at += n
        due, early, end = {}, [], []
        my_ins, side_ins, my_outs, side_outs, mine, its = parts
        side.bind(side_ins, side_outs, its)
        if prepare:
            prepare(*mine)
        for when, one in side.steps():
            slot = int(np.searchsorted(times, when))
            if when < 0:
                early.append(one)
            elif slot < len(times):
                due.setdefault(slot, []).append(one)
            else:
                end.append(one)

        step = pl.program_id(0)

        @pl.when(step == 0)
        def _():
            side.meet()
            for one in early:
                one()

        def poke(number, among):
            def choose(some):
                if len(some) == 1:

                    @pl.when(number == some[0])
                    def _():
                        for one in due[some[0]]:
                            one()
                elif some:
                    middle = len(some) // 2
                    lax.cond(number < some[middle], lambda: choose(some[:middle]), lambda: choose(some[middle:]))

            choose(sorted(at for at in among if at in due))

        body(poke, *my_ins, *my_outs, *mine)

        @pl.when(step == grid - 1)
        def _():
            for one in end:
                one()

    got = pl.pallas_call(
        kernel,
        grid=(grid,),
        in_specs=in_specs + side.in_specs,
        out_specs=out_specs + side.out_specs,
        out_shape=outs + side.outs,
        scratch_shapes=scratch + side.scratch,
        compiler_params=pltpu.CompilerParams(
            dimension_semantics=("arbitrary",), vmem_limit_bytes=VMEM_LIMIT, collective_id=ident, has_side_effects=True),
        cost_estimate=pl.CostEstimate(flops=flops, bytes_accessed=sum(a.size * a.dtype.itemsize for a in (*ins, *outs)), transcendentals=0),
        name=name,
    )(*ins, *side.ins)
    return got[: len(outs)], got[len(outs) :]


TILE = 512
FINE = 64


def scale_of(wide):
    return lax.rsqrt(jnp.mean(wide * wide, -1, keepdims=True) + 1e-6)


def turn(t, cos, sin):
    half = t.shape[-1] // 2
    a, b = t[:, :half].astype(f32), t[:, half:].astype(f32)
    return jnp.concatenate([a * cos - b * sin, b * cos + a * sin], -1).astype(bf16)


def table(tokens):
    half = HEAD // 2
    rate = np.float64(THETA) ** (-np.arange(half) / half)
    coarse, fine = (np.arange(n)[:, None] * step * rate for n, step in ((tokens // FINE, FINE), (FINE, 1)))
    return [jnp.asarray(np.stack([np.cos(a), np.sin(a)]).astype(np.float32)) for a in (coarse, fine)]


def angles(coarse_ref, fine_ref, first):
    at = pl.ds(pl.multiple_of(first // FINE, TILE // FINE), TILE // FINE)
    cos_a, sin_a = coarse_ref[0, at, :][:, None, :], coarse_ref[1, at, :][:, None, :]
    cos_b, sin_b = fine_ref[0][None], fine_ref[1][None]
    shape = (TILE, fine_ref.shape[2])
    return (cos_a * cos_b - sin_a * sin_b).reshape(shape), (sin_a * cos_b + cos_a * sin_b).reshape(shape)


def whole(shape):
    return pl.BlockSpec(shape, lambda *_: (0,) * len(shape))


def tiles(rows, columns):
    return pl.BlockSpec((rows, columns), lambda i, *_: (i, 0))


def hidden(b):
    return lax.broadcasted_iota(jnp.int32, (b, b), 0) <= lax.broadcasted_iota(jnp.int32, (b, b), 1)


def matrix(ref, first, rows):
    value = ref[:, first : first + rows, :] if len(ref.shape) == 3 else ref[:, :, first : first + rows, :]
    return value.reshape(-1, value.shape[-1])


def slots_of(tokens, layout):
    n = tokens // TILE
    return n + n * (n + 1) // 2, n * layout.at["w_gate"][2]


def forward(x, layout, coarse, fine, layers, side, ident):
    tokens, d = x.shape
    b, width = TILE, layout.width
    heads = width // HEAD
    e = HEAD**-0.5 * LOG2E
    steps = tokens // b
    _, r, parts = layout.at["w_gate"]
    ff = parts * width
    _, small = layout.span("wq", "wv")
    chips = side.devices // 2
    some = side.devices // parts
    r_down = layout.at["w_down"][1]
    look_slots, feed_slots = slots_of(tokens, layout)
    each = 2 * steps
    every_layer = [n * (look_slots + feed_slots) for n in range(layers)]
    base = [i + i * (i + 1) // 2 for i in range(steps)]
    sites = lambda *at: [n + one for n in every_layer for one in at]

    def prepare(*scratch):
        w_s, rest_s, sem = scratch[-3:]

        def load(u):
            unit = side.units[u]
            first, end = unit["span"]
            target = w_s if end <= small else rest_s
            to = first if end <= small else first - small
            return pltpu.make_async_copy(
                side.full.at[unit["layer"], :, :, pl.ds(first, end - first), :], target.at[:, :, pl.ds(to, end - first), :], sem.at[u])

        side.load = load
        side.then = lambda u: load(u).start()

    def wait(i, when, early):
        for n in range(layers):

            @pl.when(i == n * each + when)
            def _():
                for u, unit in enumerate(side.units):
                    if unit["layer"] == n and (unit["span"][1] <= small) == early:
                        side.load(u).wait()

    def body(poke, x_ref, coarse_ref, fine_ref, q_ref, k_ref, v_ref, o_ref, lse_ref, h1_ref, gate_ref, up_ref, hn_ref,
             h_s, o_s, k_s, v_s, top_s, mix_s, w_s, rest_s, sem):
        i = pl.program_id(0)
        layer, within = i // each, lax.rem(i, each)
        zero = layer * (look_slots + feed_slots)
        wait(i, 0, True)
        wait(i, steps, False)

        @pl.when(within < steps)
        def _():
            iq = within
            slot = zero + iq + iq * (iq + 1) // 2
            poke(slot, sites(*base))
            mine = pl.ds(pl.multiple_of(iq * b, b), b)

            @pl.when(layer == 0)
            def _():
                h_s[mine, :] = x_ref[:]

            wide = h_s[mine, :].astype(f32)
            a = (wide * scale_of(wide)).astype(bf16)
            cos, sin = angles(coarse_ref, fine_ref, iq * b)
            for n, (out, all_s) in enumerate(((q_ref, None), (k_ref, k_s), (v_ref, v_s))):
                t = dot(a, matrix(w_s, n * r, r)).astype(bf16)
                for m in range(heads):
                    one = t[:, head(m)]
                    one = one if n == 2 else turn(one, cos, sin)
                    out[m] = one
                    if n:
                        all_s[m, mine, :] = one
            top_s[:] = jnp.full(top_s.shape, NEG, f32)
            mix_s[:] = jnp.zeros(mix_s.shape, f32)
            ones = jnp.ones((8, b), bf16)

            def block(j, masked):
                here = pl.ds(pl.multiple_of(j * b, b), b)
                scores = [dot_last(k_s[n, here, :], q_ref[n]) for n in range(heads)]
                weights, keeps = [], []
                for n, s in enumerate(scores):
                    if masked:
                        s = jnp.where(hidden(b), s, 2 * NEG)
                    old = top_s[row(n), :]
                    top = jnp.maximum(old, s.max(axis=0, keepdims=True))
                    top_s[row(n), :] = top
                    weights.append(jnp.exp2((s - top) * e).astype(bf16))
                    keeps.append(jnp.exp2((old - top) * e))
                for n in range(heads):
                    values = jnp.concatenate([v_s[n, here, :].T, ones], axis=0)
                    mix_s[n] = mix_s[n] * keeps[n] + dot(values, weights[n])

            def seen(j):
                poke(slot + 1 + j, sites(*(base[n] + 1 + j for n in range(steps) for j in range(n))))
                block(j, False)

            loop(iq, seen)
            poke(slot + 1 + iq, sites(*(base[n] + 1 + n for n in range(steps))))
            block(iq, True)
            for n in range(heads):
                total = mix_s[n, HEAD : HEAD + 1, :]
                one = (mix_s[n, :HEAD, :] * (1 / total)).T.astype(bf16)
                o_ref[:, head(n)] = one
                o_s[mine, head(n)] = one
                lse_ref[row(n), :] = top_s[row(n), :] * HEAD**-0.5 + jnp.log(total)

        def feed(last):
            t = within - steps
            slot = zero + look_slots + parts * t
            mine = pl.ds(pl.multiple_of(t * b, b), b)
            poke(slot, sites(*(look_slots + parts * n for n in range(steps))))
            at_d, at_g, at_u = (layout.at[name][0] - small for name in ("w_down", "w_gate", "w_up"))
            h1 = h_s[mine, :] + dot(o_s[mine, :], matrix(rest_s, 0, r)).astype(bf16)
            h1_ref[:] = h1
            wide = h1.astype(f32)
            c = (wide * scale_of(wide)).astype(bf16)
            total = None
            for n in range(parts):
                if n:
                    poke(slot + n, sites(*(look_slots + parts * m + n for m in range(steps))))
                at = slice(n * width, (n + 1) * width)
                gate = dot(c, matrix(rest_s, at_g + n * r, r))
                up = dot(c, matrix(rest_s, at_u + n * r, r))
                gate_ref[:, at] = gate
                up_ref[:, at] = up
                if not last:
                    p = (gate * jax.nn.sigmoid(gate) * up).astype(bf16)
                    down = rest_s[n * some // 2 : (n + 1) * some // 2, :, at_d : at_d + r_down, :].reshape(width, d)
                    one = dot(p, down)
                    total = one if total is None else total + one
            if not last:
                h = h1 + total.astype(bf16)
                h_s[mine, :] = h
                hn_ref[:] = h

        for last in range(2):

            @pl.when((within >= steps) & ((layer == layers - 1) == bool(last)))
            def _():
                feed(last)

    which = lambda i: i // each
    early = lambda i: jnp.minimum(lax.rem(i, each), steps - 1)
    late = lambda i: jnp.maximum(lax.rem(i, each) - steps, 0)
    per_head = pl.BlockSpec((None, heads, b, HEAD), lambda i: (which(i), 0, early(i), 0))
    rows = lambda columns, when: pl.BlockSpec((None, b, columns), lambda i: (which(i), when(i), 0))
    ahead = lambda i: jnp.minimum(which(i), layers - 2)
    return run(
        body, layers * each, [x, coarse, fine],
        [pl.BlockSpec((b, d), lambda i: (jnp.minimum(i, steps - 1), 0)), whole(coarse.shape), whole(fine.shape)],
        [sds((layers, heads, tokens, HEAD), bf16)] * 3 + [sds((layers, tokens, width), bf16), sds((layers, heads, tokens), f32)]
        + [sds((layers, tokens, d), bf16)] + [sds((layers, tokens, ff), f32)] * 2 + [sds((layers - 1, tokens, d), bf16)],
        [per_head] * 3 + [rows(width, early), pl.BlockSpec((None, heads, b), lambda i: (which(i), 0, early(i)))]
        + [rows(d, late)] + [rows(ff, late)] * 2
        + [pl.BlockSpec((None, b, d), lambda i: (ahead(i), jnp.where(which(i) > ahead(i), steps - 1, late(i)), 0))],
        [pltpu.VMEM((tokens, d), bf16), pltpu.VMEM((tokens, width), bf16)] + [pltpu.VMEM((heads, tokens, HEAD), bf16)] * 2
        + [pltpu.VMEM((heads, b), f32), pltpu.VMEM((heads, HEAD + 8, b), f32)]
        + [pltpu.VMEM((chips, 2, small, width), bf16), pltpu.VMEM((chips, 2, layout.rows - small, width), bf16)]
        + [pltpu.SemaphoreType.DMA((len(side.units),))],
        side, ident, name="forward", times=range(every_layer[-1] + look_slots + feed_slots), prepare=prepare,
        flops=layers * (6 * tokens * d * width + 2 * heads * tokens * tokens * HEAD + 2 * tokens * d * (d + 3 * ff)))


def backward(x, dy, saved, full, layout, coarse, fine, side, ident):
    q, k, v, o, lse, h1, gate, up, ahead = saved
    layers, tokens, d = h1.shape
    ff, heads, width = gate.shape[2], q.shape[1], layout.width
    b, part = TILE, HEAD
    scale = HEAD**-0.5
    e = scale * LOG2E
    half, parts = tokens // b, ff // part
    blocks = half * (half + 1) // 2
    steps, slots = parts + half + 3, parts + blocks + 3
    r, r_down = layout.at["wq"][1], layout.at["w_down"][1]
    devices, chips = side.devices, side.devices // 2
    which = lambda i: layers - 1 - i // steps
    sites = lambda *at: [n * slots + one for n in range(layers) for one in at]

    def body(poke, x_ref, dy_ref, h1_ref, gate_ref, up_ref, ahead_ref, q_ref, k_ref, v_ref, o_ref, lse_ref, g_ref, u_ref, d_ref, w_ref, wo_ref,
             coarse_ref, fine_ref, dh_s, x_s, n_s, sum_s, kv_s, big_s, dq_a, dq_s, do_s, dwo_s, sem):
        i = pl.program_id(0)
        layer, within = which(i), lax.rem(i, steps)
        zero = (i // steps) * slots
        by_gu, by_d, by_small = side.term
        dk_s, dv_s = big_s.at[0], big_s.at[1]
        k_s, v_s = kv_s.at[0], kv_s.at[1]
        p_s, dgate_s, dup_s, t_s = k_s.at[0], k_s.at[1], v_s.at[0], k_s

        def tile(t):
            return pl.ds(pl.multiple_of(t * b, b), b)

        def chunk(layer, f):
            at, slot = pl.ds(pl.multiple_of(f * part, part), part), lax.rem(f, 2)
            return [pltpu.make_async_copy(ref.at[layer, :, at], big_s.at[slot, n], sem.at[slot, n]) for n, ref in enumerate((gate_ref, up_ref))]

        states = lambda: pltpu.make_async_copy(h1_ref.at[layer], x_s, sem.at[2, 0])
        first = lambda: pltpu.make_async_copy(dy_ref, dh_s, sem.at[2, 1])

        def inputs(start):
            for n in range(layers):

                @pl.when(layer == n)
                def _():
                    copy = pltpu.make_async_copy(ahead_ref.at[n - 1] if n else x_ref, x_s, sem.at[2, 0])
                    copy.start() if start else copy.wait()

        def norm(t):
            wide = x_s[tile(t), :].astype(f32)
            n_s[tile(t), :] = (wide * scale_of(wide)).astype(bf16)

        def norm_back(t):
            wide = x_s[tile(t), :].astype(f32)
            size = scale_of(wide)
            dn = sum_s[tile(t), :].astype(bf16).astype(f32)
            back = size * dn - wide * (size * size * size * jnp.mean(dn * wide, -1, keepdims=True))
            dh_s[tile(t), :] = dh_s[tile(t), :] + back.astype(bf16)

        @pl.when(within < parts)
        def _():
            f = within
            poke(zero + f, sites(*range(parts)))

            @pl.when(f == 0)
            def _():
                states().start()
                sum_s[:] = jnp.zeros(sum_s.shape, f32)

            @pl.when(i == 0)
            def _():
                first().start()
                for copy in chunk(layer, f):
                    copy.start()
                first().wait()

            for copy in chunk(layer, f):
                copy.wait()

            @pl.when(f < parts - 1)
            def _():
                for copy in chunk(layer, f + 1):
                    copy.start()

            @pl.when(f == 0)
            def _():
                states().wait()
                loop(half, norm)

            slot = lax.rem(f, 2)
            for t in range(half):
                here = slice(t * b, (t + 1) * b)
                dp = dot_last(dh_s[here, :], d_ref[:].reshape(part, d)).astype(bf16).astype(f32)
                gate, up = big_s[slot, 0, here, :], big_s[slot, 1, here, :]
                s = jax.nn.sigmoid(gate)
                soft = gate * s
                dup = (dp * soft).astype(bf16)
                dgate = (dp * up * (s + soft * (1 - s))).astype(bf16)
                p_s[here, :] = (soft * up).astype(bf16)
                dgate_s[here, :] = dgate
                dup_s[here, :] = dup
                sum_s[here, :] += dot_last(dgate, g_ref[:].reshape(d, part)) + dot_last(dup, u_ref[:].reshape(d, part))

            some = part // (2 * r_down)
            by_d[0, pl.ds(f * some, some)] = dot_first(p_s[:], dh_s[:]).astype(bf16).reshape(some, 2, r_down, d)
            at = pl.ds(pl.multiple_of(f * part, part), part)
            by_gu[0, :, :, :, at] = dot_first(n_s[:], dgate_s[:]).astype(bf16).reshape(chips, 2, r, part)
            by_gu[1, :, :, :, at] = dot_first(n_s[:], dup_s[:]).astype(bf16).reshape(chips, 2, r, part)

            @pl.when(f == parts - 1)
            def _():
                loop(half, norm_back)
                inputs(True)

        @pl.when((within >= parts) & (within < parts + half))
        def _():
            m = within - parts
            slot = zero + parts + m * (m + 1) // 2
            poke(slot, sites(*(parts + n * (n + 1) // 2 for n in range(half))))
            mine = tile(m)
            k_s[:, mine, :] = k_ref[:]
            v_s[:, mine, :] = v_ref[:]
            do_s[:] = dot_last(dh_s[mine, :], matrix(wo_ref, 0, r)).astype(bf16)
            one = dot_first(o_ref[:], dh_s[mine, :])
            dwo_s[:] = jnp.where(m == 0, one, dwo_s[:] + one)
            deltas = []
            for n in range(heads):
                cut = head(n)
                deltas.append((do_s[:, cut].astype(f32) * o_ref[:, cut].astype(f32)).T.sum(axis=0, keepdims=True))

            def block(j, diagonal):
                here = tile(j)
                dos = [do_s[:, head(n)] for n in range(heads)]
                scores = [dot_last(k_s[n, here, :], q_ref[n]) for n in range(heads)]
                dps = [dot_last(v_s[n, here, :], dos[n]) for n in range(heads)]
                for n in range(heads):
                    p = jnp.exp2(scores[n] * e - lse_ref[row(n), :] * LOG2E)
                    if diagonal:
                        p = jnp.where(hidden(b), p, 0.0)
                    ds = (p * (dps[n] - deltas[n])).astype(bf16)
                    for total, one in ((dv_s.at[n, here, :], dot(p.astype(bf16), dos[n])), (dk_s.at[n, here, :], dot(ds, q_ref[n])),
                                       (dq_s.at[n], dot(k_s[n, here, :].T, ds))):
                        total[:] = one if diagonal else total[:] + one

            block(m, True)

            def seen(j):
                poke(slot + 1 + j, sites(*(parts + n * (n + 1) // 2 + 1 + j for n in range(half) for j in range(n))))
                block(j, False)

            loop(m, seen)
            for n in range(heads):
                dq_a[n, mine, :] = (dq_s[n] * scale).T.astype(bf16)

        @pl.when(within == parts + half - 1)
        def _():
            by_small[0] = dwo_s[:].astype(bf16).reshape(chips, 2, r, d)
            inputs(False)
            loop(half, norm)

        @pl.when(within >= parts + half)
        def _():
            n = within - parts - half
            poke(zero + parts + blocks + n, sites(*range(parts + blocks, slots)))

            def made(number, source):
                @pl.when(n == number)
                def _():
                    def some(t):
                        cos, sin = (None, None) if number == 0 else angles(coarse_ref, fine_ref, t * b)
                        for m in range(heads):
                            one = source(m, tile(t))
                            t_s[m, tile(t), :] = one if number == 0 else turn(one, cos, -sin)

                    loop(half, some)

            made(0, lambda m, at: dv_s[m, at, :].astype(bf16))
            made(1, lambda m, at: (dk_s[m, at, :] * scale).astype(bf16))
            made(2, lambda m, at: dq_a[m, at, :])

            @pl.when((n == 2) & (layer > 0))
            def _():
                for copy in chunk(layer - 1, 0):
                    copy.start()

            for m in range(heads):
                cut = head(m)
                by_small[1 + n, :, :, :, cut] = dot_first(n_s[:], t_s[m]).astype(bf16).reshape(chips, 2, r, HEAD)

            @pl.when(layer > 0)
            def _():
                rows = pl.ds(pl.multiple_of((2 - n) * r, r), r)

                def back(t):
                    w = w_ref[:, rows, :].reshape(d, width)
                    one = sum(dot_last(t_s[m, tile(t), :], w[:, head(m)]) for m in range(heads))
                    sum_s[tile(t), :] = jnp.where(n == 0, one, sum_s[tile(t), :] + one)

                loop(half, back)

                @pl.when(n == 2)
                def _():
                    loop(half, norm_back)

    def spec(shape, index):
        return pl.BlockSpec((None,) + shape, lambda i: (which(i), *index(lax.rem(i, steps))))

    now = lambda w: jnp.minimum(w, parts - 1)
    query = lambda w: jnp.clip(w - parts, 0, half - 1)
    block = spec((heads, b, HEAD), lambda w: (0, query(w), 0))
    per = width // part

    def slab(name):
        first = layout.at[name][0] // r
        return spec((devices, r, part), lambda w: (0, first + now(w) // per, lax.rem(now(w), per)))

    def matrices(first, last):
        start, end = layout.span(first, last)
        return spec((devices, end - start, width), lambda w: (0, start // (end - start), 0))

    at_d = layout.at["w_down"][0]
    return run(
        body, layers * steps, [x, dy, h1, gate, up, ahead, q, k, v, o, lse, full, full, full, full, full, coarse, fine],
        [ANY] * 6 + [block] * 3 + [spec((b, width), lambda w: (query(w), 0)), spec((heads, b), lambda w: (0, query(w)))]
        + [slab("w_gate"), slab("w_up"), spec((part // r_down, r_down, width), lambda w: (now(w), at_d // r_down, 0))]
        + [matrices("wq", "wv"), matrices("wo", "wo"), whole(coarse.shape), whole(fine.shape)],
        [], [],
        [pltpu.VMEM((tokens, d), bf16)] * 3 + [pltpu.VMEM((tokens, d), f32), pltpu.VMEM((2, heads, tokens, HEAD), bf16)]
        + [pltpu.VMEM((2, 2, tokens, part), f32), pltpu.VMEM((heads, tokens, HEAD), bf16), pltpu.VMEM((heads, HEAD, b), f32)]
        + [pltpu.VMEM((b, width), bf16), pltpu.VMEM((width, d), f32), pltpu.SemaphoreType.DMA((3, 2))],
        side, ident, times=range(layers * slots), name="backward",
        flops=layers * (12 * tokens * d * ff + 5 * heads * tokens * tokens * HEAD + 16 * tokens * d * width))[1]


def adamw(weights, m, v, gradients):
    arrays, at = [], {}
    for array in (piece[0] for one in gradients for layer in one for piece in layer):
        if id(array) not in at:
            at[id(array)] = len(arrays)
            arrays.append(array)
    layers = len(gradients[0])

    def kernel(*refs):
        left = iter(refs)
        w_refs, m_refs, v_refs, g_refs, new_w, new_m, new_v = (
            [next(left) for _ in some] for some in (weights, m, v, arrays, weights, weights, weights))
        layer = pl.program_id(0)

        def update(number):
            for i, pieces in enumerate(gradients):
                for array, index, first in pieces[number]:
                    here = slice(first, first + array.shape[2])
                    g = g_refs[at[id(array)]][index].astype(f32)
                    w = w_refs[i][:, here].astype(f32)
                    moment = 0.9 * m_refs[i][:, here] + 0.1 * g
                    square = 0.95 * v_refs[i][:, here] + 0.05 * g * g
                    step = moment * lax.rsqrt(square + 1e-8) + 0.1 * w
                    new_w[i][:, here] = (w - 0.02 * step).astype(bf16)
                    new_m[i][:, here] = moment
                    new_v[i][:, here] = square

        for number in range(layers):
            pl.when(layer == number)(functools.partial(update, number))

    kinds = (bf16, f32, f32)
    one_layer = [pl.BlockSpec((None, *w.shape[1:]), lambda n: (n, 0, 0)) for _ in kinds for w in weights]
    return pl.pallas_call(
        kernel,
        grid=(layers,),
        in_specs=one_layer + [whole(array.shape) for array in arrays],
        out_specs=one_layer,
        out_shape=[sds(w.shape, kind) for kind in kinds for w in weights],
        compiler_params=pltpu.CompilerParams(vmem_limit_bytes=VMEM_LIMIT),
        name="adamw",
    )(*weights, *m, *v, *arrays)


def every(start, gap, count):
    return [start + gap * n for n in range(count)]


def forward_plan():
    ring, fetched = every(-90, 10, 7), [4, 6, 9, 11, 14, 14, 19, 24]
    plan = [(0, "wq", "wv", False, ring), (1, "wq", "wv", True, fetched)]
    for n, names in enumerate((("wo", "w_down"), ("w_gate", "w_gate"), ("w_up", "w_up"))):
        plan.append((0, *names, "fine", every(11 * n - 79, 10, 4) + [1, 6, 11]))
        plan.append((1, *names, True, [4, 9, 14, 19, 24, 24, 37, 41]))
    return plan


def backward_plan(parts, blocks, rows, columns):
    low, high, down, small = (0, columns // 2), (columns // 2, columns), (0, rows), (0, rows)
    two, one, half, each = (0, 2), (0, 1), parts // 2, parts + blocks + 3
    after = [parts + n for n in (0, 2, 5, 8)]
    plan = [(0, "low", 0, two, low, [*range(half, parts + 1), after[1]])]
    plan += [(0, name, at, m_, which, after + [each - 2, each]) for name, at, m_, which in (("high", 0, two, high), ("down", 1, one, down))]
    plan += [(0, "small", 2, (0, 4), small, [each + n for n in (0, 2, 4, 6, parts, parts + 2)])]
    plan += [(1, "low", 0, two, low, [each + n for n in (*range(half, parts + 1), after[1])])]
    now = [each + n for n in after]
    end = 2 * each
    plan += [(1, name, at, m_, which, now + [end - 2, end + 0.7]) for name, at, m_, which in (("high", 0, two, high), ("down", 1, one, down))]
    for name, first, last, start in (("small", 0, 2, -2), ("k", 2, 3, -1), ("q", 3, 4, -0.1)):
        due = [end + start, end + start + 1]
        plan.append((1, name, 2, (first, last), small, due + every(end + 1 + first / 10, 1, 4)))
    return plan


def gather(groups, devices, weights, plan):
    layout = Layout(weights)
    units = [dict(layer=layer, span=layout.span(first, last), share=share, at=at) for layer, first, last, share, at in plan]
    return Gather(groups, devices, weights, units)


def solution(mesh):
    groups, devices = mesh.shape["rep"], mesh.shape["dp"]

    def step(x, dy, *arrays):
        weights, m, v = (arrays[i : i + 7] for i in (0, 7, 14))
        layers = weights[0].shape[0]
        layout = Layout(weights)
        h = x[0]
        tokens, d = h.shape
        coarse, fine = table(tokens)
        idents = iter(range(64))

        side = gather(groups, devices, weights, forward_plan())
        saved, (full,) = forward(h, layout, coarse, fine, layers, side, next(idents))
        ff, half = saved[6].shape[2], tokens // TILE
        parts = ff // HEAD
        buffers = [(m_, devices // 2, 2, w.shape[1], w.shape[2]) for m_, w in zip((2, 1, 4), (weights[i] for i in map(NAMES.index, ("w_up", "w_down", "wq"))))]
        units, where = [], {}
        for n, name, buffer, m_, columns, at in backward_plan(parts, half * (half + 1) // 2, d, ff):
            where[layers - 1 - n, name] = len(units)
            units.append(dict(buffer=buffer, m=m_, columns=columns, at=at, after=where.get((layers - n, name))))
        got = backward(h, dy[0], saved, full.reshape(layers, devices, *full.shape[3:]), layout, coarse, fine,
                       Scatter(groups, devices, buffers, units), next(idents))

        def pieces(number, name):
            one = lambda unit, index, first=0: (got[where[number, unit]], index, first)
            if name in ("w_gate", "w_up"):
                return [one(unit, int(name == "w_up"), first) for unit, first in (("low", 0), ("high", ff // 2))]
            if name == "w_down":
                return [one("down", 0)]
            place = ("wo", "wv", "wk", "wq").index(name)
            own = name[1:] if (number, name[1:]) in where else "small"
            return [one(own, 0 if own != "small" else place)]

        return tuple(adamw(weights, m, v, [[pieces(number, name) for number in range(layers)] for name in NAMES]))

    states, cut = P(("rep", "dp")), P(None, "dp")
    return jax.shard_map(
        step,
        mesh=mesh,
        in_specs=(states, states) + (cut,) * 21,
        out_specs=(P("rep", "dp"),) * 21,
        check_vma=False,
    )
```
